32 devices in a mesh: gx: 16 (over z, x, core), gy: 2 (over y).
Axes of the slice: x: 2, y: 2, z: 4, core: 2. Of those that a mesh axis runs over, the one named last changes fastest.
Arguments:
- right_side: float32 [16, 4, 8, 8, 128], P('gx', 'gy'), may hold values from -6 to 6
- inverse_blocks: float32 [16, 4, 8, 128, 128], P('gx', 'gy'), may hold values from -1.7 to 1.7
- couple_x: float32 [16, 4, 8, 8, 128], P('gx', 'gy'), may hold values from -0.127 to -0.105
- couple_y: float32 [16, 4, 8, 8, 128], P('gx', 'gy'), may hold values from -0.007 to -0.003
- couple_z: float32 [16, 4, 8, 8, 8], P('gx', 'gy'), may hold values from -0.75 to 0.75
Outputs:
- solution: float32 [16, 4, 8, 8, 128], P('gx', 'gy')
The draws below stay inside these ranges and needn't reach their ends.
All inputs are finite; a program needn't handle non-finite values.
Results may differ from the reference program's by a relative error of at most 0.0001.
Values sent between devices are 32-bit elements; how exact they have to be, the bound alone decides.
A program may use at most 64 MiB of HBM per device.

```python
import math
import jax
import jax.numpy as jnp
from jax import lax

NC = 8
ZB = 8
NRHS = 8
BR = 128
NZ = 128
NX = 16
NY = 4


def draw_inverse_blocks(key, part):
    key_diag, key_rest = jax.random.split(key)
    scales = jax.random.uniform(key_diag, (NX, NY, ZB, BR, 1), jnp.float32, 0.6, 1.4)
    spread = jax.random.normal(key_rest, (NX, NY, ZB, BR, BR), jnp.float32) * (0.35 / math.sqrt(BR))
    return spread + scales * jnp.eye(BR, dtype=jnp.float32)


def draw_couple_x(key, part):
    inner = jax.random.fold_in(key, 11)
    magnitude = jax.random.uniform(inner, (NX, NY, NC, NC, NZ), jnp.float32, 0.105, 0.127)
    return -magnitude


def draw_couple_y(key, part):
    inner = jax.random.fold_in(key, 23)
    magnitude = jax.random.uniform(inner, (NX, NY, NC, NC, NZ), jnp.float32, 0.003, 0.007)
    return -magnitude


def block_scale(key, extent, cuts, low, high):
    gain = 1.0
    for dim, shards_of in cuts:
        draws = jax.random.uniform(jax.random.fold_in(jax.random.fold_in(key, 6), dim), (shards_of,), jnp.float32, low / len(cuts), high / len(cuts))
        gain = gain * jnp.repeat(jnp.exp(draws), extent[dim] // shards_of).reshape((-1,) + (1,) * (len(extent) - 1 - dim))
    return gain


def centred(key, shape, deviation, most, cuts=(), held_as=jnp.bfloat16):
    gain = block_scale(key, shape, cuts, -0.22, 0.18) if cuts else 1.0
    result = jax.random.normal(key, shape, jnp.float32) * deviation * gain
    return jnp.minimum(jnp.maximum(result, -most), most).astype(held_as)


def setup_inputs(seed: int = 0) -> dict:
    streams_of = jax.random.split(jax.random.key(seed), 6)
    return {
        "right_side": centred(streams_of[0], (NX, NY, NRHS, NC, NZ), 1.0, 6.0, ((0, 16), (1, 2)), jnp.float32),
        "inverse_blocks": draw_inverse_blocks(jax.random.fold_in(streams_of[5], 71), 0),
        "couple_x": draw_couple_x(jax.random.fold_in(streams_of[5], 71), 0),
        "couple_y": draw_couple_y(jax.random.fold_in(streams_of[5], 71), 0),
        "couple_z": centred(streams_of[4], (NX, NY, ZB, NC, NC), 0.125, 0.75, ((0, 16), (1, 2)), jnp.float32),
    }


exact_mode = lax.Precision.HIGHEST


def couple(matrix, values_in):
    return jnp.einsum("cdz,ndz->ncz", matrix, values_in, precision=exact_mode)


def reference(right_side, inverse_blocks, couple_x, couple_y, couple_z):
    vectors = right_side.shape[2]
    components = right_side.shape[3]
    z_cells = right_side.shape[4]
    segments = inverse_blocks.shape[2]
    seg_len = z_cells // segments

    def segment_step(z_prior, inputs):
        seg_piece, inverse, corner = inputs
        head_row = seg_piece[:, :, 0] - jnp.einsum("cd,nd->nc", corner, z_prior, precision=exact_mode)
        seg_piece = jnp.concatenate([head_row[:, :, None], seg_piece[:, :, 1:]], axis=2)
        flattened = seg_piece.reshape(vectors, components * seg_len)
        solved = jnp.dot(flattened, inverse.T, precision=exact_mode, preferred_element_type=jnp.float32)
        solved = solved.reshape(vectors, components, seg_len)
        return solved[:, :, -1], solved

    def column_step(y_prior, inputs):
        partial_value, inverse, along_y, corner = inputs
        partial_value = partial_value - couple(along_y, y_prior)
        pieces = partial_value.reshape(vectors, components, segments, seg_len).transpose(2, 0, 1, 3)
        zero_state = jnp.zeros((vectors, components), jnp.float32)
        _, solved = lax.scan(segment_step, zero_state, (pieces, inverse, corner))
        column = solved.transpose(1, 2, 0, 3).reshape(vectors, components, z_cells)
        return column, column

    def plane_step(x_prior, inputs):
        rhs_plane, inverse, along_x, along_y, corner = inputs
        partial_value = rhs_plane - jnp.einsum("ycdz,yndz->yncz", along_x, x_prior, precision=exact_mode)
        zero_column = jnp.zeros((vectors, components, z_cells), jnp.float32)
        _, x_plane = lax.scan(column_step, zero_column, (partial_value, inverse, along_y, corner))
        return x_plane, x_plane

    zero_plane = jnp.zeros(right_side.shape[1:], jnp.float32)
    _, solution = lax.scan(plane_step, zero_plane, (right_side, inverse_blocks, couple_x, couple_y, couple_z))
    return solution
```

```python
import functools
import jax
import jax.numpy as jnp
from jax import lax
from jax.experimental import pallas as pl
from jax.experimental.pallas import tpu as pltpu
from jax.sharding import PartitionSpec as P

MESH = pl.DeviceIdType.MESH
PAIR = 2
OWN = PAIR - 1
EARLY = 3
LAG = 3
F32 = jnp.float32
BF16 = jnp.bfloat16


def roll(tile, shift):
    shift = shift % tile.shape[1]
    return tile if shift == 0 else pltpu.roll(tile, shift, 1)


def unskew(skewed, seg_len):
    count = len(skewed)
    group = lax.broadcasted_iota(jnp.int32, skewed[0].shape, 1) // seg_len
    rows = []
    for s in range(count):
        acc = skewed[0]
        for c in range(1, count):
            acc = jnp.where(group == (s + c) % count, skewed[c], acc)
        rows.append(roll(acc, -s * seg_len))
    return rows


def relayout(tiles, seg_len):
    return unskew([roll(t, c * seg_len) for c, t in enumerate(tiles)], seg_len)


def split(value):
    high = value.astype(BF16)
    return high, (value - high.astype(F32)).astype(BF16)


def add_up(terms):
    while len(terms) > 1:
        terms = [sum(terms[i:i + 2][1:], terms[i]) for i in range(0, len(terms), 2)]
    return terms[0]


def finish(seg_len, rows, out):
    for y in range(rows.shape[0]):
        tiles = relayout([rows[y, s] for s in range(rows.shape[1])], seg_len)
        for c, tile in enumerate(tiles):
            out[0, y, :, c, :] = tile


def kernel(
    nx, ny, dims,
    rhs, inv, cx, cy, cz, out,
    rhs_v, inv_v, cx_v, cy_v, cz_v, zpad, w_v, r_v, nx_v, ny_v, nz_v, k_v, g_v, xin, yin, sol_v,
    load_sem, push_sem, move_sem, x_sem, y_sem, send_sem,
):
    yl, vectors, comps, segs, seg_len = dims
    width = comps * seg_len
    gx = lax.axis_index("gx")
    gy = lax.axis_index("gy")
    group = gx // PAIR
    slot = gx % PAIR
    groups = nx // PAIR
    origin = jnp.logical_and(group == 0, gy == 0)
    barrier = pltpu.get_barrier_semaphore()
    small = ((rhs, rhs_v), (cx, cx_v), (cy, cy_v), (cz, cz_v))
    count = len(small)

    def pieces(h):
        return [(a.at[0], b.at[h]) for a, b in small]

    def load(k):
        a, b = pieces(OWN)[k]
        return pltpu.make_async_copy(a, b, load_sem.at[k])

    def load_block(s):
        return pltpu.make_async_copy(inv.at[0, :, s], inv_v.at[OWN, :, s], load_sem.at[count + s])

    def push(k):
        a, b = pieces(0)[k]
        return pltpu.make_async_remote_copy(
            src_ref=a, dst_ref=b, send_sem=push_sem.at[k], recv_sem=move_sem.at[k],
            device_id=(gx + OWN, gy), device_id_type=MESH,
        )

    def push_block(s):
        return pltpu.make_async_remote_copy(
            src_ref=inv.at[0, :, s], dst_ref=inv_v.at[0, :, s], send_sem=push_sem.at[count + s],
            recv_sem=move_sem.at[count + s], device_id=(gx + OWN, gy), device_id_type=MESH,
        )

    def arrive(h, k):
        load(k).wait() if h == OWN else push(k).wait_recv()

    def arrive_block(h, s):
        load_block(s).wait() if h == OWN else push_block(s).wait_recv()

    def greet(dx, dy):
        pl.semaphore_signal(barrier, inc=1, device_id=(gx + dx, gy + dy), device_id_type=MESH)

    def greet_if(cond, dx, dy):
        pl.when(cond)(functools.partial(greet, dx, dy))

    def send(kind, src, dst, sem, dx, dy):
        return pltpu.make_async_remote_copy(
            src_ref=src, dst_ref=dst, send_sem=send_sem.at[kind], recv_sem=sem,
            device_id=(gx + dx, gy + dy), device_id_type=MESH,
        )

    def send_x(kind, y, s, dx):
        return send(kind, out.at[y, s], xin.at[y, s], x_sem.at[y, s], dx, 0)

    def send_y(kind, src, h, s, dx):
        return send(kind, src.at[yl - 1, s], yin.at[h, s], y_sem.at[h, s], dx, 1)

    def settle(ref, kind):
        pltpu.make_async_copy(ref, ref, send_sem.at[kind]).wait()

    def start_loads():
        for k in range(count):
            load(k).start()
        for s in range(segs):
            load_block(s).start()

    lane = lax.broadcasted_iota(jnp.int32, (comps, width), 1)
    diagonal = (
        lax.broadcasted_iota(jnp.int32, (seg_len, width), 0)
        == lax.broadcasted_iota(jnp.int32, (seg_len, width), 1) % seg_len
    )

    def prepare(h, direct, with_x=True):
        def turn(tile, c):
            return pltpu.roll(tile, comps - c, 0) if direct and c else tile

        for k in range(count):
            arrive(h, k)
        for y in range(yl):
            for s in range(segs):
                zpad[y, s * seg_len:s * seg_len + comps, 0:comps] = cz_v[h, y, s]
        flipped = [zpad[y].T[0:comps, :] for y in range(yl)]
        for y in range(yl):
            for s, row in enumerate(relayout([rhs_v[h, y, :, c, :] for c in range(comps)], seg_len)):
                r_v[h, y, s] = row
            for s, row in enumerate(relayout([turn(cy_v[h, y, c], c) for c in range(comps)], seg_len)):
                ny_v[h, y, s] = row
            if with_x:
                for s, row in enumerate(relayout([turn(cx_v[h, y, c], c) for c in range(comps)], seg_len)):
                    nx_v[h, y, s] = row
        for y in range(yl):
            for s, row in enumerate(unskew([roll(flipped[y], c * (seg_len - 1)) for c in range(comps)], seg_len)):
                nz_v[h, y, s] = jnp.where(lane % seg_len == 0, row, 0.0)

    def couple(value, rows):
        return add_up([roll(value, -r * seg_len) * rows[r:r + 1, :] for r in range(comps)])

    def combine(both):
        top, bottom = both[0:vectors], both[vectors:2 * vectors]
        return (top[:, width:] + bottom[:, width:]) + (bottom[:, :width] + top[:, :width])

    def relax(y, s, y_prior):
        partial = r_v[OWN, y, s]
        if y_prior is not None:
            partial = partial - couple(y_prior, ny_v.at[OWN, y, s])
        left = split(partial)
        if s > 0:
            left = left + split(nz_v[OWN, y, s])
        both = lax.dot_general(
            jnp.concatenate(left, 0), jnp.concatenate(split(inv_v[OWN, y, s]), 0), (((1,), (1,)), ((), ())),
            preferred_element_type=F32,
        )
        return combine(both), combine(both[2 * vectors:]) if s > 0 else None

    def ends(tile):
        return [
            jnp.broadcast_to(tile[:, (d + 1) * seg_len - 1:(d + 1) * seg_len], (vectors, width))
            for d in range(comps)
        ]

    def climb(relaxed, prior):
        free, along = relaxed
        if prior is not None:
            free = free - add_up([e * along[d:d + 1, :] for d, e in enumerate(ends(prior))])
        return free

    def dense(tile):
        return jnp.concatenate(
            [
                jnp.concatenate(
                    [
                        jnp.where(diagonal, jnp.broadcast_to(part[d:d + 1], (seg_len, width)), 0.0).astype(BF16)
                        for d in range(comps)
                    ],
                    0,
                )
                for part in (p.astype(F32) for p in split(tile))
            ],
            1,
        )

    def product(h, y, s):
        high, low = split(inv_v[h, y, s])
        block = jnp.concatenate([jnp.concatenate([high, high], 1), jnp.concatenate([low, low], 1)], 0)
        head = jnp.concatenate(split(jnp.concatenate([r_v[h, y, s], nz_v[h, y, s]], 0)), 1)
        left = jnp.concatenate([head, dense(nx_v[h, y, s]), dense(ny_v[h, y, s])], 0)
        both = lax.dot_general(left, block, (((1,), (1,)), ((), ())), preferred_element_type=F32)
        return both[:, :width] + both[:, width:]

    first_row = vectors + comps

    def keep(y, s, base, rows):
        high, low = split(rows)
        w_v[y, s, base:base + rows.shape[0], 0:width] = high
        w_v[y, s, base:base + rows.shape[0], width:2 * width] = low

    def fold(h, i, y, s):
        total = product(h, y, s)
        k_v[i, y, s] = total[0:vectors]
        g_v[i, y, s] = total[vectors:first_row]
        keep(y, s, i * 2 * width, total[first_row:])

    def fold_column(h, i, unroll):
        for s in range(segs):
            arrive_block(h, s)

        def fold_row(s, carry):
            for y in range(yl):
                fold(h, i, y, s)
            return carry

        lax.fori_loop(0, segs, fold_row, 0, unroll=unroll)

    def fold_pair(y, s):
        lower_total = product(0, y, s)
        k_v[0, y, s] = lower_total[0:vectors]
        g_v[0, y, s] = lower_total[vectors:first_row]
        keep(y, s, 0, lower_total[first_row:])
        upper_total = product(OWN, y, s)
        g_v[2, y, s] = upper_total[vectors:first_row]
        keep(y, s, 4 * width, upper_total[first_row + width:])
        high, low = split(upper_total[first_row:first_row + width])
        high_low = jnp.concatenate([high, low], 1)
        both = jnp.dot(
            jnp.concatenate(split(lower_total), 1), jnp.concatenate([high_low, high_low], 0),
            preferred_element_type=F32,
        )
        total = both[:, :width] + both[:, width:]
        k_v[1, y, s] = upper_total[0:vectors] - total[0:vectors]
        g_v[1, y, s] = total[vectors:first_row]
        keep(y, s, 2 * width, total[first_row:])

    def along_z(parts, i, y, s):
        return add_up([p * g_v[i, y, s, d:d + 1, :] for d, p in enumerate(parts)])

    def stack(*tiles):
        parts = [split(t) for t in tiles]
        return jnp.concatenate(
            [jnp.concatenate([p[0] for p in parts], 1), jnp.concatenate([p[1] for p in parts], 1)], 0
        )

    def times(left, y, s, base, rows):
        return jnp.dot(left, w_v[y, s, base:base + rows, :], preferred_element_type=F32)

    def solve(i, y, s, sol, x_prior, y_prior):
        if y_prior is None:
            both = times(stack(x_prior), y, s, i * 2 * width, width)
        else:
            both = times(stack(x_prior, y_prior), y, s, i * 2 * width, 2 * width)
        acc = k_v[i, y, s]
        if s > 0:
            acc = acc - along_z(ends(sol[y, s - 1]), i, y, s)
        return acc - combine(both)

    def solve_pair(cells, priors, send_on):
        lefts = [(stack(x, y0), stack(y1)) for x, y0, y1 in priors]
        upper_both = [
            times(left, y, s, 2 * width, 2 * width) - times(left1, y, s, 4 * width, width)
            for (left, left1), (y, s) in zip(lefts, cells)
        ]
        lower_both = [times(left, y, s, 0, 2 * width) for (left, _), (y, s) in zip(lefts, cells)]
        lower_accs = []
        for (y, s), upper_b in zip(cells, upper_both):
            lower_acc = k_v[0, y, s]
            upper_acc = k_v[1, y, s]
            if s > 0:
                lower_ends, upper_ends = ends(sol_v[y, s - 1]), ends(out[y, s - 1])
                upper_acc = (upper_acc - along_z(upper_ends, 2, y, s)) + along_z(lower_ends, 1, y, s)
                lower_acc = lower_acc - along_z(lower_ends, 0, y, s)
            lower_accs.append(lower_acc)
            out[y, s] = upper_acc + combine(upper_b)
        send_on(cells)
        for (y, s), lower_acc, lower_b in zip(cells, lower_accs, lower_both):
            sol_v[y, s] = lower_acc - combine(lower_b)

    def cells_at(t, columns):
        return [
            (x, y, t - x - y) for x in range(columns) for y in range(yl) if 0 <= t - x - y < segs
        ]

    def first_lower():
        start_loads()
        zpad[...] = jnp.zeros_like(zpad)
        prepare(OWN, True, with_x=False)
        for s in range(segs):
            arrive_block(OWN, s)
        relaxed = {(0, s): relax(0, s, None) for s in range(segs)}
        values = {}
        pl.semaphore_wait(barrier, 1 + (2 if ny > 1 else 0))
        for t in range(segs + (yl - 1) * LAG):
            for y in range(1, yl):
                s = t - 1 - (y - 1) * LAG
                if 0 <= s < segs:
                    relaxed[y, s] = relax(y, s, values[y - 1, s])
            ready = [(y, t - y * LAG) for y in range(yl) if 0 <= t - y * LAG < segs]
            for y, s in ready:
                values[y, s] = climb(relaxed[y, s], values.get((y, s - 1)))
                out[y, s] = values[y, s]
            for y, s in ready:
                send_x(0, y, s, OWN).start()
            for y, s in ready:
                if ny > 1 and y == yl - 1:
                    send_y(2, out, 0, s, OWN).start()
                    send_y(3, out, 0, s, 0).start()
        settle(xin, 0)
        if ny > 1:
            settle(yin.at[0], 2)
            settle(yin.at[0], 3)

    def first_upper():
        start_loads()
        greet(-OWN, 0)
        zpad[...] = jnp.zeros_like(zpad)
        prepare(OWN, False)
        fold_column(OWN, 0, 4)
        peers = (2 if groups > 1 else 0) + (1 if ny > 1 else 0)
        if peers:
            pl.semaphore_wait(barrier, peers)
        for t in range(segs + yl - 1):
            cells = [(y, t - y) for y in range(yl) if 0 <= t - y < segs]
            for y, s in cells:
                send_x(0, y, s, OWN).wait_recv()
            values = [solve(0, y, s, out, xin[y, s], out[y - 1, s] if y > 0 else None) for y, s in cells]
            for (y, s), value in zip(cells, values):
                out[y, s] = value
            if groups > 1:
                for kind, dx in ((0, PAIR), (1, OWN)):
                    for y, s in cells:
                        send_x(kind, y, s, dx).start()
            for y, s in cells:
                if ny > 1 and y == yl - 1:
                    send_y(4, out, OWN, s, 0).start()
        if groups > 1:
            settle(xin, 0)
            settle(xin, 1)
        if ny > 1:
            settle(yin.at[0], 4)

    def clear():
        zpad[...] = jnp.zeros_like(zpad)

        @pl.when(group == 0)
        def _():
            xin[...] = jnp.zeros_like(xin)

        @pl.when(gy == 0)
        def _():
            yin[...] = jnp.zeros_like(yin)

    def wait_x(cells):
        if not cells:
            return

        @pl.when(group > 0)
        def _():
            for y, s in cells:
                send_x(0, y, s, PAIR).wait_recv()

    def wait_y(cells):
        if not cells:
            return

        @pl.when(gy > 0)
        def _():
            for h, s in cells:
                send_y(0, out, h, s, 0).wait_recv()

    def lower():
        start_loads()
        greet_if(group > 0, -OWN, 0)
        greet_if(jnp.logical_and(gy > 0, jnp.logical_or(group > 0, gy > 1)), OWN, -1)
        greet_if(jnp.logical_and(gy == 1, group == 0), 0, -1)
        pl.semaphore_wait(barrier, 1)
        for k in range(count):
            push(k).start()
        for s in range(segs):
            push_block(s).start()
        clear()
        prepare(OWN, False)

        fold_column(OWN, 0, 2)
        for t in range(segs + yl - 1):
            cells = cells_at(t, 1)
            wait_x([(y, s) for _, y, s in cells])
            wait_y([(0, s) for _, y, s in cells if y == 0])
            values = [solve(0, y, s, out, xin[y, s], yin[0, s] if y == 0 else out[y - 1, s]) for _, y, s in cells]
            for (_, y, s), value in zip(cells, values):
                out[y, s] = value
        for k in range(count):
            push(k).wait_send()
        for s in range(segs):
            push_block(s).wait_send()

    right = group < groups - 1
    above = gy < ny - 1

    def enter_upper():
        start_loads()
        greet(-OWN, 0)
        greet_if(group > 0, -PAIR, 0)
        greet_if(gy > 0, 0, -1)
        greet_if(jnp.logical_and(gy == 1, group == 0), -OWN, -1)
        clear()

    def meet_upper():
        @pl.when(jnp.logical_or(right, above))
        def _():
            pl.semaphore_wait(barrier, jnp.where(right, 2, 0) + jnp.where(above, 2, 0))

    def send_right(done):
        if not done:
            return

        @pl.when(right)
        def _():
            for kind, dx in ((0, PAIR), (1, OWN)):
                for y, s in done:
                    send_x(kind, y, s, dx).start()

    def send_above(done):
        if any(y == yl - 1 for _, y, _ in done):
            @pl.when(above)
            def _():
                for h, y, s in done:
                    if y == yl - 1:
                        if h == OWN:
                            send_y(4, out, OWN, s, 0).start()
                        else:
                            send_y(2, sol_v, 0, s, 0).start()
                            send_y(3, sol_v, 0, s, -OWN).start()

    def leave_upper():
        @pl.when(right)
        def _():
            settle(xin, 0)
            settle(xin, 1)

        @pl.when(above)
        def _():
            for kind in range(2, 5):
                settle(yin.at[0], kind)

    def upper_plain():
        enter_upper()
        for h in reversed(range(PAIR)):
            prepare(h, False)
            fold_column(h, h, 4)
        meet_upper()
        sols = (sol_v, out)
        for t in range(segs + PAIR + yl - 2):
            cells = [(x, y, t - x - y) for x in reversed(range(PAIR)) for y in range(yl) if 0 <= t - x - y < segs]
            wait_x([(y, s) for x, y, s in cells if x == 0])
            wait_y([(x, s) for x, y, s in cells if y == 0])
            values = [
                solve(
                    x, y, s, sols[x], xin[y, s] if x == 0 else sol_v[y, s],
                    yin[x, s] if y == 0 else sols[x][y - 1, s],
                )
                for x, y, s in cells
            ]
            for (x, y, s), value in zip(cells, values):
                if x == OWN:
                    out[y, s] = value
            send_right([(y, s) for x, y, s in cells if x == OWN])
            for (x, y, s), value in zip(cells, values):
                if x != OWN:
                    sol_v[y, s] = value
            send_above(cells)
        leave_upper()

    def upper_folded():
        enter_upper()
        for h in reversed(range(PAIR)):
            prepare(h, False)

        for h in reversed(range(PAIR)):
            for s in range(segs):
                arrive_block(h, s)

        def fold_all(s, carry):
            for y in range(yl):
                fold_pair(y, s)
            return carry

        lax.fori_loop(0, segs, fold_all, 0, unroll=2)
        meet_upper()
        for t in range(segs + yl - 1):
            cells = [(y, s) for _, y, s in cells_at(t, 1)]
            wait_x(cells)
            wait_y([(h, s) for y, s in cells if y == 0 for h in range(PAIR)])
            solve_pair(
                cells,
                [
                    (xin[y, s], yin[0, s] if y == 0 else sol_v[y - 1, s], yin[OWN, s] if y == 0 else out[y - 1, s])
                    for y, s in cells
                ],
                send_right,
            )
            send_above([(h, y, s) for y, s in cells for h in reversed(range(PAIR))])
        leave_upper()

    early = group < EARLY
    is_upper = jnp.logical_and(jnp.logical_not(origin), slot == OWN)
    pl.when(jnp.logical_and(origin, slot == 0))(first_lower)
    pl.when(jnp.logical_and(origin, slot == OWN))(first_upper)
    pl.when(jnp.logical_and(jnp.logical_not(origin), slot == 0))(lower)
    pl.when(jnp.logical_and(is_upper, early))(upper_plain)
    pl.when(jnp.logical_and(is_upper, jnp.logical_not(early)))(upper_folded)


def local(nx, ny, right_side, inverse_blocks, couple_x, couple_y, couple_z):
    _, yl, vectors, comps, cells = right_side.shape
    segs = inverse_blocks.shape[2]
    seg_len = cells // segs
    width = comps * seg_len
    lead = (PAIR, yl)
    rows = pltpu.VMEM(lead + (segs, comps, width), F32)
    vectors_v = pltpu.VMEM(lead + (segs, vectors, width), F32)
    vmem = pl.BlockSpec(memory_space=pltpu.VMEM)
    any_spec = pl.BlockSpec(memory_space=pl.ANY)
    solved = pl.pallas_call(
        functools.partial(kernel, nx, ny, (yl, vectors, comps, segs, seg_len)),
        out_shape=pltpu.VMEM((yl, segs, vectors, width), F32),
        in_specs=[any_spec] * 5,
        out_specs=vmem,
        scratch_shapes=[
            pltpu.VMEM(lead + right_side.shape[2:], F32),
            pltpu.VMEM(lead + inverse_blocks.shape[2:], F32),
            pltpu.VMEM(lead + couple_x.shape[2:], F32),
            pltpu.VMEM(lead + couple_y.shape[2:], F32),
            pltpu.VMEM(lead + couple_z.shape[2:], F32),
            pltpu.VMEM((yl, segs * seg_len, width), F32),
            pltpu.VMEM((yl, segs, 5 * width, 2 * width), BF16),
            vectors_v, rows, rows, rows, vectors_v,
            pltpu.VMEM((PAIR + 1, yl, segs, comps, width), F32),
            pltpu.VMEM((yl, segs, vectors, width), F32),
            pltpu.VMEM((PAIR, segs, vectors, width), F32),
            pltpu.VMEM((yl, segs, vectors, width), F32),
            pltpu.SemaphoreType.DMA((4 + segs,)),
            pltpu.SemaphoreType.DMA((4 + segs,)),
            pltpu.SemaphoreType.DMA((4 + segs,)),
            pltpu.SemaphoreType.DMA((yl, segs)),
            pltpu.SemaphoreType.DMA((PAIR, segs)),
            pltpu.SemaphoreType.DMA((5,)),
        ],
        compiler_params=pltpu.CompilerParams(collective_id=0, has_side_effects=True),
        name="forward_solve",
    )(right_side, inverse_blocks, couple_x, couple_y, couple_z)
    return pl.pallas_call(
        functools.partial(finish, seg_len),
        out_shape=jax.ShapeDtypeStruct(right_side.shape, F32),
        in_specs=[vmem],
        out_specs=vmem,
        name="natural_layout",
    )(pltpu.with_memory_space_constraint(solved, pltpu.VMEM))


def solution(mesh):
    spec = P("gx", "gy", None, None, None)
    return jax.shard_map(
        functools.partial(local, mesh.shape["gx"], mesh.shape["gy"]),
        mesh=mesh, in_specs=(spec,) * 5, out_specs=spec, check_vma=False,
    )
```

```python
import functools
import jax
import jax.numpy as jnp
from jax import lax
from jax.experimental import pallas as pl
from jax.experimental.pallas import tpu as pltpu
from jax.sharding import PartitionSpec as P

MESH = pl.DeviceIdType.MESH
PAIR = 2
OWN = PAIR - 1
EARLY = 3
LAG = 3
F32 = jnp.float32
BF16 = jnp.bfloat16


def roll(tile, shift):
    shift = shift % tile.shape[1]
    return tile if shift == 0 else pltpu.roll(tile, shift, 1)


def unskew(skewed, seg_len):
    count = len(skewed)
    group = lax.broadcasted_iota(jnp.int32, skewed[0].shape, 1) // seg_len
    rows = []
    for s in range(count):
        acc = skewed[0]
        for c in range(1, count):
            acc = jnp.where(group == (s + c) % count, skewed[c], acc)
        rows.append(roll(acc, -s * seg_len))
    return rows


def relayout(tiles, seg_len):
    return unskew([roll(t, c * seg_len) for c, t in enumerate(tiles)], seg_len)


def split(value):
    high = value.astype(BF16)
    return high, (value - high.astype(F32)).astype(BF16)


def add_up(terms):
    while len(terms) > 1:
        terms = [sum(terms[i:i + 2][1:], terms[i]) for i in range(0, len(terms), 2)]
    return terms[0]


def finish(seg_len, rows, out):
    for y in range(rows.shape[0]):
        tiles = relayout([rows[y, s] for s in range(rows.shape[1])], seg_len)
        for c, tile in enumerate(tiles):
            out[0, y, :, c, :] = tile


def kernel(
    nx, ny, dims,
    rhs, inv, cx, cy, cz, out,
    rhs_v, inv_v, cx_v, cy_v, cz_v, zpad, w_v, r_v, nx_v, ny_v, nz_v, k_v, g_v, xin, yin, sol_v,
    load_sem, push_sem, move_sem, x_sem, y_sem, send_sem,
):
    yl, vectors, comps, segs, seg_len = dims
    width = comps * seg_len
    gx = lax.axis_index("gx")
    gy = lax.axis_index("gy")
    group = gx // PAIR
    slot = gx % PAIR
    groups = nx // PAIR
    origin = jnp.logical_and(group == 0, gy == 0)
    right = group < groups - 1
    above = gy < ny - 1
    inner = jnp.logical_and(group > 0, right)
    before_last = group == groups - 2
    barrier = pltpu.get_barrier_semaphore()
    small = ((rhs, rhs_v), (cx, cx_v), (cy, cy_v), (cz, cz_v))
    count = len(small)

    def pieces(h):
        return [(a.at[0], b.at[h]) for a, b in small]

    def load(k):
        a, b = pieces(OWN)[k]
        return pltpu.make_async_copy(a, b, load_sem.at[k])

    def load_block(s):
        return pltpu.make_async_copy(inv.at[0, :, s], inv_v.at[OWN, :, s], load_sem.at[count])

    def push(k):
        a, b = pieces(0)[k]
        return pltpu.make_async_remote_copy(
            src_ref=a, dst_ref=b, send_sem=push_sem.at[k], recv_sem=move_sem.at[k],
            device_id=(gx + OWN, gy), device_id_type=MESH,
        )

    def push_block(s):
        return pltpu.make_async_remote_copy(
            src_ref=inv.at[0, :, s], dst_ref=inv_v.at[0, :, s], send_sem=push_sem.at[count],
            recv_sem=move_sem.at[count], device_id=(gx + OWN, gy), device_id_type=MESH,
        )

    def arrive(h, k):
        load(k).wait() if h == OWN else push(k).wait_recv()

    def drain(ref, sem):
        pltpu.make_async_copy(ref, ref, sem).wait()

    def arrive_blocks(h):
        drain(inv_v.at[h], (load_sem if h == OWN else move_sem).at[count])

    def greet(dx, dy):
        pl.semaphore_signal(barrier, inc=1, device_id=(gx + dx, gy + dy), device_id_type=MESH)

    def greet_if(cond, dx, dy):
        pl.when(cond)(functools.partial(greet, dx, dy))

    def send(kind, src, dst, sem, dx, dy):
        return pltpu.make_async_remote_copy(
            src_ref=src, dst_ref=dst, send_sem=send_sem.at[kind], recv_sem=sem,
            device_id=(gx + dx, gy + dy), device_id_type=MESH,
        )

    def send_x(y, s, dx):
        return send(0 if dx == PAIR else 1, out.at[y, s], xin.at[y, s], x_sem.at[y + s], dx, 0)

    def send_y(src, h, s, dx):
        return send(2 + h, src.at[yl - 1, s], yin.at[h, s], y_sem.at[h, s], dx, 1)

    def hand_down(y, s):
        return send(4, xin.at[y, s], xin.at[y, s], x_sem.at[y + s], -OWN, 0)

    def take_x(cells):
        drain(xin.at[0, 0:len(cells)], x_sem.at[sum(cells[0])])

    def start_loads():
        for k in range(count):
            load(k).start()
        for s in range(segs):
            load_block(s).start()

    lane = lax.broadcasted_iota(jnp.int32, (comps, width), 1)
    diagonal = (
        lax.broadcasted_iota(jnp.int32, (seg_len, width), 0)
        == lax.broadcasted_iota(jnp.int32, (seg_len, width), 1) % seg_len
    )

    def arrive_small(h):
        for k in range(count):
            arrive(h, k)

    def prepare_r(h):
        for y in range(yl):
            for s, row in enumerate(relayout([rhs_v[h, y, :, c, :] for c in range(comps)], seg_len)):
                r_v[h, y, s] = row

    def prepare_yz(h, turned):
        for y in range(yl):
            for s in range(segs):
                zpad[y, s * seg_len:s * seg_len + comps, 0:comps] = cz_v[h, y, s]
        flipped = [zpad[y].T[0:comps, :] for y in range(yl)]
        for y in range(yl):
            tiles = [pltpu.roll(cy_v[h, y, c], comps - c, 0) if turned and c else cy_v[h, y, c] for c in range(comps)]
            for s, row in enumerate(relayout(tiles, seg_len)):
                ny_v[h, y, s] = row
        for y in range(yl):
            for s, row in enumerate(unskew([roll(flipped[y], c * (seg_len - 1)) for c in range(comps)], seg_len)):
                nz_v[h, y, s] = jnp.where(lane % seg_len == 0, row, 0.0)

    def prepare(h):
        arrive_small(h)
        prepare_r(h)
        for y in range(yl):
            for s, row in enumerate(relayout([cx_v[h, y, c] for c in range(comps)], seg_len)):
                nx_v[h, y, s] = row
        prepare_yz(h, False)

    def couple(value, rows):
        return add_up([roll(value, -r * seg_len) * rows[r:r + 1, :] for r in range(comps)])

    def combine(both):
        top, bottom = both[0:vectors], both[vectors:2 * vectors]
        return (top[:, width:] + bottom[:, width:]) + (bottom[:, :width] + top[:, :width])

    def relax(y, s, y_prior):
        partial = r_v[OWN, y, s]
        if y_prior is not None:
            partial = partial - couple(y_prior, ny_v.at[OWN, y, s])
        left = split(partial)
        if s > 0:
            left = left + split(nz_v[OWN, y, s])
        both = lax.dot_general(
            jnp.concatenate(left, 0), jnp.concatenate(split(inv_v[OWN, y, s]), 0), (((1,), (1,)), ((), ())),
            preferred_element_type=F32,
        )
        return combine(both), combine(both[2 * vectors:]) if s > 0 else None

    def ends(tile):
        return [
            jnp.broadcast_to(tile[:, (d + 1) * seg_len - 1:(d + 1) * seg_len], (vectors, width))
            for d in range(comps)
        ]

    def climb(relaxed, prior):
        free, along = relaxed
        if prior is not None:
            free = free - add_up([e * along[d:d + 1, :] for d, e in enumerate(ends(prior))])
        return free

    def dense(tile):
        return jnp.concatenate(
            [
                jnp.concatenate(
                    [
                        jnp.where(diagonal, jnp.broadcast_to(part[d:d + 1], (seg_len, width)), 0.0).astype(BF16)
                        for d in range(comps)
                    ],
                    0,
                )
                for part in (p.astype(F32) for p in split(tile))
            ],
            1,
        )

    def product(h, y, s):
        high, low = split(inv_v[h, y, s])
        block = jnp.concatenate([jnp.concatenate([high, high], 1), jnp.concatenate([low, low], 1)], 0)
        head = jnp.concatenate(split(jnp.concatenate([r_v[h, y, s], nz_v[h, y, s]], 0)), 1)
        left = jnp.concatenate([head, dense(nx_v[h, y, s]), dense(ny_v[h, y, s])], 0)
        both = lax.dot_general(left, block, (((1,), (1,)), ((), ())), preferred_element_type=F32)
        return both[:, :width] + both[:, width:]

    first_row = vectors + comps

    def keep(y, s, base, rows):
        high, low = split(rows)
        w_v[y, s, base:base + rows.shape[0], 0:width] = high
        w_v[y, s, base:base + rows.shape[0], width:2 * width] = low

    def fold(h, i, y, s):
        total = product(h, y, s)
        k_v[i, y, s] = total[0:vectors]
        g_v[i, y, s] = total[vectors:first_row]
        keep(y, s, i * 2 * width, total[first_row:])

    def fold_column(h, i, unroll):
        arrive_blocks(h)

        def fold_row(s, carry):
            for y in range(yl):
                fold(h, i, y, s)
            return carry

        lax.fori_loop(0, segs, fold_row, 0, unroll=unroll)

    def fold_pair(y, s):
        lower_total = product(0, y, s)
        k_v[0, y, s] = lower_total[0:vectors]
        g_v[0, y, s] = lower_total[vectors:first_row]
        keep(y, s, 0, lower_total[first_row:])
        upper_total = product(OWN, y, s)
        g_v[2, y, s] = upper_total[vectors:first_row]
        keep(y, s, 4 * width, upper_total[first_row + width:])
        high, low = split(upper_total[first_row:first_row + width])
        high_low = jnp.concatenate([high, low], 1)
        both = jnp.dot(
            jnp.concatenate(split(lower_total), 1), jnp.concatenate([high_low, high_low], 0),
            preferred_element_type=F32,
        )
        total = both[:, :width] + both[:, width:]
        k_v[1, y, s] = upper_total[0:vectors] - total[0:vectors]
        g_v[1, y, s] = total[vectors:first_row]
        keep(y, s, 2 * width, total[first_row:])

    def along_z(parts, i, y, s):
        return add_up([p * g_v[i, y, s, d:d + 1, :] for d, p in enumerate(parts)])

    def stack(*tiles):
        parts = [split(t) for t in tiles]
        return jnp.concatenate(
            [jnp.concatenate([p[0] for p in parts], 1), jnp.concatenate([p[1] for p in parts], 1)], 0
        )

    def times(left, y, s, base, rows):
        return jnp.dot(left, w_v[y, s, base:base + rows, :], preferred_element_type=F32)

    def solve(cells, priors, sols, late=None):
        both = [
            times(stack(x), y, s, i * 2 * width, width) if y_prior is None
            else times(stack(x, y_prior), y, s, i * 2 * width, 2 * width)
            for (i, y, s), (x, y_prior) in zip(cells, priors)
        ]
        below = [ends(sols[i][y, s - 1]) if s > 0 else None for i, y, s in cells]
        if late is not None:
            late()
        values = []
        for (i, y, s), b, z in zip(cells, both, below):
            acc = k_v[i, y, s]
            if z is not None:
                acc = acc - along_z(z, i, y, s)
            values.append(acc - combine(b))
        return values

    def solve_pair(cells, priors, late, send_on):
        lefts = [(stack(x, y0), stack(y1)) for x, y0, y1 in priors]
        upper_both = [
            times(left, y, s, 2 * width, 2 * width) - times(left1, y, s, 4 * width, width)
            for (left, left1), (y, s) in zip(lefts, cells)
        ]
        lower_both = [times(left, y, s, 0, 2 * width) for (left, _), (y, s) in zip(lefts, cells)]
        below = [(ends(sol_v[y, s - 1]), ends(out[y, s - 1])) if s > 0 else None for y, s in cells]
        late()
        lower_accs = []
        for (y, s), upper_b, z in zip(cells, upper_both, below):
            lower_acc = k_v[0, y, s]
            upper_acc = k_v[1, y, s]
            if z is not None:
                lower_ends, upper_ends = z
                upper_acc = (upper_acc - along_z(upper_ends, 2, y, s)) + along_z(lower_ends, 1, y, s)
                lower_acc = lower_acc - along_z(lower_ends, 0, y, s)
            lower_accs.append(lower_acc)
            out[y, s] = upper_acc + combine(upper_b)
        send_on()
        for (y, s), lower_acc, lower_b in zip(cells, lower_accs, lower_both):
            sol_v[y, s] = lower_acc - combine(lower_b)

    def wave(t):
        return [(y, t - y) for y in range(yl) if 0 <= t - y < segs]

    def first_lower():
        start_loads()
        zpad[...] = jnp.zeros_like(zpad)
        arrive_small(OWN)
        prepare_r(OWN)
        arrive_blocks(OWN)
        relaxed = {(0, 0): relax(0, 0, None)}
        values = {}
        pl.semaphore_wait(barrier, 1 + (2 if ny > 1 else 0))

        def pass_on(ready):
            for y, s in ready:
                values[y, s] = climb(relaxed[y, s], values.get((y, s - 1)))
                out[y, s] = values[y, s]
            for y, s in ready:
                send_x(y, s, OWN).start()
            for y, s in ready:
                if ny > 1 and y == yl - 1:
                    send_y(out, 0, s, OWN).start()
                    send_y(out, 0, s, 0).start()

        pass_on([(0, 0)])
        prepare_yz(OWN, True)
        for s in range(1, segs):
            relaxed[0, s] = relax(0, s, None)
        for t in range(1, segs + (yl - 1) * LAG):
            for y in range(1, yl):
                s = t - 1 - (y - 1) * LAG
                if 0 <= s < segs:
                    relaxed[y, s] = relax(y, s, values[y - 1, s])
            pass_on([(y, t - y * LAG) for y in range(yl) if 0 <= t - y * LAG < segs])
        drain(xin, send_sem.at[1])
        if ny > 1:
            drain(yin, send_sem.at[2])

    def first_upper():
        start_loads()
        greet(-OWN, 0)
        zpad[...] = jnp.zeros_like(zpad)
        prepare(OWN)
        fold_column(OWN, 0, 4)
        peers = (groups > 1) + (groups == 2) + (ny > 1)
        if peers:
            pl.semaphore_wait(barrier, peers)
        def later(cells):
            if groups == 2:
                for y, s in cells:
                    send_x(y, s, OWN).start()
            for y, s in cells:
                if ny > 1 and y == yl - 1:
                    send_y(out, OWN, s, 0).start()

        for t in range(segs + yl - 1):
            cells = wave(t)
            take_x(cells)
            values = solve(
                [(0, y, s) for y, s in cells],
                [(xin[y, s], out[y - 1, s] if y > 0 else None) for y, s in cells],
                (out,), functools.partial(later, wave(t - 1)),
            )
            for (y, s), value in zip(cells, values):
                out[y, s] = value
            if groups > 1:
                for y, s in cells:
                    send_x(y, s, PAIR).start()
        later(wave(segs + yl - 2))
        if groups > 1:
            drain(xin, send_sem.at[0])
        if groups == 2:
            drain(xin, send_sem.at[1])
        if ny > 1:
            drain(yin.at[0], send_sem.at[2 + OWN])

    def clear():
        zpad[...] = jnp.zeros_like(zpad)

        @pl.when(group == 0)
        def _():
            xin[...] = jnp.zeros_like(xin)

        @pl.when(gy == 0)
        def _():
            yin[...] = jnp.zeros_like(yin)

    def wait_x(cells):
        if not cells:
            return

        @pl.when(group > 0)
        def _():
            take_x(cells)

    def wait_y(cells):
        if not cells:
            return

        @pl.when(gy > 0)
        def _():
            for h, s in cells:
                send_y(out, h, s, 0).wait_recv()

    def lower():
        start_loads()
        greet_if(jnp.logical_and(group > 0, jnp.logical_not(right)), -OWN, 0)
        greet_if(inner, OWN, 0)
        greet_if(jnp.logical_and(gy > 0, jnp.logical_or(group > 0, gy > 1)), OWN, -1)
        greet_if(jnp.logical_and(gy == 1, group == 0), 0, -1)
        pl.semaphore_wait(barrier, 1)
        for k in range(count):
            push(k).start()
        for s in range(segs):
            push_block(s).start()
        clear()
        prepare(OWN)

        fold_column(OWN, 0, 2)
        for t in range(segs + yl - 1):
            cells = wave(t)
            wait_x(cells)
            wait_y([(0, s) for y, s in cells if y == 0])
            values = solve(
                [(0, y, s) for y, s in cells],
                [(xin[y, s], yin[0, s] if y == 0 else out[y - 1, s]) for y, s in cells], (out,),
            )
            for (y, s), value in zip(cells, values):
                out[y, s] = value
        for k in range(count):
            push(k).wait_send()
        drain(inv_v.at[OWN], push_sem.at[count])

    def enter_upper():
        start_loads()
        greet(-OWN, 0)
        greet_if(group > 0, -PAIR, 0)
        greet_if(gy > 0, 0, -1)
        greet_if(jnp.logical_and(gy == 1, group == 0), -OWN, -1)
        clear()

    def meet_upper():
        @pl.when(jnp.logical_or(right, above))
        def _():
            peers = jnp.where(right, 1, 0) + jnp.where(inner, 1, 0) + jnp.where(before_last, 1, 0)
            pl.semaphore_wait(barrier, peers + jnp.where(above, 2, 0))

    def send_down(cells):
        if cells:
            @pl.when(inner)
            def _():
                for y, s in cells:
                    hand_down(y, s).start()

    def send_right(done):
        if any(h == OWN for h, _, _ in done):
            @pl.when(right)
            def _():
                for h, y, s in done:
                    if h == OWN:
                        send_x(y, s, PAIR).start()

    def send_later(done):
        if any(y == yl - 1 for _, y, _ in done):
            @pl.when(above)
            def _():
                for h, y, s in done:
                    if y == yl - 1:
                        send_y(out if h == OWN else sol_v, h, s, 0).start()
                for h, y, s in done:
                    if y == yl - 1 and h != OWN:
                        send_y(sol_v, h, s, -OWN).start()

        if any(h == OWN for h, _, _ in done):
            @pl.when(before_last)
            def _():
                for h, y, s in done:
                    if h == OWN:
                        send_x(y, s, OWN).start()

    def leave_upper():
        for cond, kind in ((right, 0), (before_last, 1), (inner, 4)):
            pl.when(cond)(functools.partial(drain, xin, send_sem.at[kind]))

        @pl.when(above)
        def _():
            drain(yin, send_sem.at[2])
            drain(yin.at[0], send_sem.at[2 + OWN])

    def upper_plain():
        enter_upper()
        for h in reversed(range(PAIR)):
            prepare(h)
            fold_column(h, h, 4)
        meet_upper()
        sols = (sol_v, out)

        def cells_at(t):
            return [(x, y, t - x - y) for x in reversed(range(PAIR)) for y in range(yl) if 0 <= t - x - y < segs]

        def late(t):
            send_down([(y, s) for x, y, s in cells_at(t) if x == 0])

        steps = segs + PAIR + yl - 2
        for t in range(steps):
            cells = cells_at(t)
            wait_x([(y, s) for x, y, s in cells if x == 0])
            wait_y([(x, s) for x, y, s in cells if y == 0])
            values = solve(
                cells,
                [
                    (xin[y, s] if x == 0 else sol_v[y, s], yin[x, s] if y == 0 else sols[x][y - 1, s])
                    for x, y, s in cells
                ],
                sols, functools.partial(late, t),
            )
            for (x, y, s), value in zip(cells, values):
                if x == OWN:
                    out[y, s] = value
            send_right(cells)
            for (x, y, s), value in zip(cells, values):
                if x != OWN:
                    sol_v[y, s] = value
            send_later(cells)
        leave_upper()

    def upper_folded():
        enter_upper()
        for h in reversed(range(PAIR)):
            prepare(h)

        for h in reversed(range(PAIR)):
            arrive_blocks(h)

        def fold_all(s, carry):
            for y in range(yl):
                fold_pair(y, s)
            return carry

        lax.fori_loop(0, segs, fold_all, 0, unroll=2)
        meet_upper()
        def both_of(cells):
            return [(h, y, s) for y, s in cells for h in reversed(range(PAIR))]

        def late(t):
            send_down(wave(t))

        for t in range(segs + yl - 1):
            cells = wave(t)
            wait_x(cells)
            wait_y([(h, s) for y, s in cells if y == 0 for h in range(PAIR)])
            solve_pair(
                cells,
                [
                    (xin[y, s], yin[0, s] if y == 0 else sol_v[y - 1, s], yin[OWN, s] if y == 0 else out[y - 1, s])
                    for y, s in cells
                ],
                functools.partial(late, t), functools.partial(send_right, both_of(cells)),
            )
            send_later(both_of(cells))
        leave_upper()

    early = group < EARLY
    is_upper = jnp.logical_and(jnp.logical_not(origin), slot == OWN)
    pl.when(jnp.logical_and(origin, slot == 0))(first_lower)
    pl.when(jnp.logical_and(origin, slot == OWN))(first_upper)
    pl.when(jnp.logical_and(jnp.logical_not(origin), slot == 0))(lower)
    pl.when(jnp.logical_and(is_upper, early))(upper_plain)
    pl.when(jnp.logical_and(is_upper, jnp.logical_not(early)))(upper_folded)


def local(nx, ny, right_side, inverse_blocks, couple_x, couple_y, couple_z):
    _, yl, vectors, comps, cells = right_side.shape
    segs = inverse_blocks.shape[2]
    seg_len = cells // segs
    width = comps * seg_len
    lead = (PAIR, yl)
    rows = pltpu.VMEM(lead + (segs, comps, width), F32)
    vectors_v = pltpu.VMEM(lead + (segs, vectors, width), F32)
    vmem = pl.BlockSpec(memory_space=pltpu.VMEM)
    any_spec = pl.BlockSpec(memory_space=pl.ANY)
    solved = pl.pallas_call(
        functools.partial(kernel, nx, ny, (yl, vectors, comps, segs, seg_len)),
        out_shape=pltpu.VMEM((yl, segs, vectors, width), F32),
        in_specs=[any_spec] * 5,
        out_specs=vmem,
        scratch_shapes=[
            pltpu.VMEM(lead + right_side.shape[2:], F32),
            pltpu.VMEM(lead + inverse_blocks.shape[2:], F32),
            pltpu.VMEM(lead + couple_x.shape[2:], F32),
            pltpu.VMEM(lead + couple_y.shape[2:], F32),
            pltpu.VMEM(lead + couple_z.shape[2:], F32),
            pltpu.VMEM((yl, segs * seg_len, width), F32),
            pltpu.VMEM((yl, segs, 5 * width, 2 * width), BF16),
            vectors_v, rows, rows, rows, vectors_v,
            pltpu.VMEM((PAIR + 1, yl, segs, comps, width), F32),
            pltpu.VMEM((yl, segs, vectors, width), F32),
            pltpu.VMEM((PAIR, segs, vectors, width), F32),
            pltpu.VMEM((yl, segs, vectors, width), F32),
            pltpu.SemaphoreType.DMA((5,)),
            pltpu.SemaphoreType.DMA((5,)),
            pltpu.SemaphoreType.DMA((5,)),
            pltpu.SemaphoreType.DMA((segs + yl - 1,)),
            pltpu.SemaphoreType.DMA((PAIR, segs)),
            pltpu.SemaphoreType.DMA((5,)),
        ],
        compiler_params=pltpu.CompilerParams(collective_id=0, has_side_effects=True),
        name="forward_solve",
    )(right_side, inverse_blocks, couple_x, couple_y, couple_z)
    return pl.pallas_call(
        functools.partial(finish, seg_len),
        out_shape=jax.ShapeDtypeStruct(right_side.shape, F32),
        in_specs=[vmem],
        out_specs=vmem,
        name="natural_layout",
    )(pltpu.with_memory_space_constraint(solved, pltpu.VMEM))


def solution(mesh):
    spec = P("gx", "gy", None, None, None)
    return jax.shard_map(
        functools.partial(local, mesh.shape["gx"], mesh.shape["gy"]),
        mesh=mesh, in_specs=(spec,) * 5, out_specs=spec, check_vma=False,
    )
```

```python
import functools
import jax
import jax.numpy as jnp
from jax import lax
from jax.experimental import pallas as pl
from jax.experimental.pallas import tpu as pltpu
from jax.sharding import PartitionSpec as P

MESH = pl.DeviceIdType.MESH
PAIR = 2
OWN = PAIR - 1
EARLY = 3
LAG = 3
CHUNK = 2
F32 = jnp.float32
BF16 = jnp.bfloat16


def roll(tile, shift):
    shift = shift % tile.shape[1]
    return tile if shift == 0 else pltpu.roll(tile, shift, 1)


def unskew(skewed, seg_len):
    count = len(skewed)
    group = lax.broadcasted_iota(jnp.int32, skewed[0].shape, 1) // seg_len
    rows = []
    for s in range(count):
        acc = skewed[0]
        for c in range(1, count):
            acc = jnp.where(group == (s + c) % count, skewed[c], acc)
        rows.append(roll(acc, -s * seg_len))
    return rows


def relayout(tiles, seg_len):
    return unskew([roll(t, c * seg_len) for c, t in enumerate(tiles)], seg_len)


def split(value):
    high = value.astype(BF16)
    return high, (value - high.astype(F32)).astype(BF16)


def add_up(terms):
    while len(terms) > 1:
        terms = [sum(terms[i:i + 2][1:], terms[i]) for i in range(0, len(terms), 2)]
    return terms[0]


def finish(seg_len, rows, out):
    for y in range(rows.shape[0]):
        tiles = relayout([rows[y, s] for s in range(rows.shape[1])], seg_len)
        for c, tile in enumerate(tiles):
            out[0, y, :, c, :] = tile


def kernel(
    nx, ny, dims,
    rhs, inv, cx, cy, cz, out,
    rhs_v, inv_v, cx_v, cy_v, cz_v, zpad, w_v, r_v, nx_v, ny_v, nz_v, k_v, g_v, xin, yin, sol_v,
    load_sem, push_sem, move_sem, x_sem, y_sem, send_sem, ready_sem,
):
    yl, vectors, comps, segs, seg_len = dims
    width = comps * seg_len
    gx = lax.axis_index("gx")
    gy = lax.axis_index("gy")
    group = gx // PAIR
    slot = gx % PAIR
    groups = nx // PAIR
    origin = jnp.logical_and(group == 0, gy == 0)
    right = group < groups - 1
    above = gy < ny - 1
    inner = jnp.logical_and(group > 0, right)
    before_last = group == groups - 2
    barrier = pltpu.get_barrier_semaphore()
    small = ((rhs, rhs_v), (cx, cx_v), (cy, cy_v), (cz, cz_v))
    count = len(small)

    def pieces(h):
        return [(a.at[0], b.at[h]) for a, b in small]

    def load(k):
        a, b = pieces(OWN)[k]
        return pltpu.make_async_copy(a, b, load_sem.at[k])

    def load_block(s):
        return pltpu.make_async_copy(inv.at[0, :, s], inv_v.at[OWN, :, s], load_sem.at[count])

    def push(k):
        a, b = pieces(0)[k]
        return pltpu.make_async_remote_copy(
            src_ref=a, dst_ref=b, send_sem=push_sem.at[k], recv_sem=move_sem.at[k],
            device_id=(gx + OWN, gy), device_id_type=MESH,
        )

    def push_block(s):
        return pltpu.make_async_remote_copy(
            src_ref=inv.at[0, :, s], dst_ref=inv_v.at[0, :, s], send_sem=push_sem.at[count],
            recv_sem=move_sem.at[count + s // CHUNK], device_id=(gx + OWN, gy), device_id_type=MESH,
        )

    def arrive(h, k):
        load(k).wait() if h == OWN else push(k).wait_recv()

    def drain(ref, sem):
        pltpu.make_async_copy(ref, ref, sem).wait()

    def arrive_blocks():
        drain(inv_v.at[OWN], load_sem.at[count])

    def arrive_chunk(p):
        drain(inv_v.at[0, :, 0:CHUNK], move_sem.at[count + p])

    def greet(dx, dy):
        pl.semaphore_signal(barrier, inc=1, device_id=(gx + dx, gy + dy), device_id_type=MESH)

    def greet_if(cond, dx, dy):
        pl.when(cond)(functools.partial(greet, dx, dy))

    def send(kind, src, dst, sem, dx, dy):
        return pltpu.make_async_remote_copy(
            src_ref=src, dst_ref=dst, send_sem=send_sem.at[kind], recv_sem=sem,
            device_id=(gx + dx, gy + dy), device_id_type=MESH,
        )

    def send_x(y, s, dx):
        return send(0 if dx == PAIR else 1, out.at[y, s], xin.at[y, s], x_sem.at[y + s], dx, 0)

    def send_y(src, h, s, dx):
        return send(2 + h, src.at[yl - 1, s], yin.at[h, s], y_sem.at[h, s], dx, 1)

    def hand_down(y, s):
        return send(4, xin.at[y, s], xin.at[y, s], x_sem.at[y + s], -OWN, 0)

    def take_x(cells):
        drain(xin.at[0, 0:len(cells)], x_sem.at[sum(cells[0])])

    def start_loads():
        for k in range(count):
            load(k).start()
        for s in range(segs):
            load_block(s).start()

    lane = lax.broadcasted_iota(jnp.int32, (comps, width), 1)
    diagonal = (
        lax.broadcasted_iota(jnp.int32, (seg_len, width), 0)
        == lax.broadcasted_iota(jnp.int32, (seg_len, width), 1) % seg_len
    )

    def arrive_small(h):
        for k in range(count):
            arrive(h, k)

    def prepare_r(h):
        for y in range(yl):
            for s, row in enumerate(relayout([rhs_v[h, y, :, c, :] for c in range(comps)], seg_len)):
                r_v[h, y, s] = row

    def prepare_y(h, turned=False):
        for y in range(yl):
            tiles = [pltpu.roll(cy_v[h, y, c], comps - c, 0) if turned and c else cy_v[h, y, c] for c in range(comps)]
            for s, row in enumerate(relayout(tiles, seg_len)):
                ny_v[h, y, s] = row

    def prepare_z(h):
        for y in range(yl):
            for s in range(segs):
                zpad[y, s * seg_len:s * seg_len + comps, 0:comps] = cz_v[h, y, s]
        flipped = [zpad[y].T[0:comps, :] for y in range(yl)]
        for y in range(yl):
            for s, row in enumerate(unskew([roll(flipped[y], c * (seg_len - 1)) for c in range(comps)], seg_len)):
                nz_v[h, y, s] = jnp.where(lane % seg_len == 0, row, 0.0)

    def prepare(h):
        arrive_small(h)
        prepare_z(h)
        prepare_r(h)
        for y in range(yl):
            for s, row in enumerate(relayout([cx_v[h, y, c] for c in range(comps)], seg_len)):
                nx_v[h, y, s] = row
        prepare_y(h)

    def couple(value, rows):
        return add_up([roll(value, -r * seg_len) * rows[r:r + 1, :] for r in range(comps)])

    def combine(both):
        top, bottom = both[0:vectors], both[vectors:2 * vectors]
        return (top[:, width:] + bottom[:, width:]) + (bottom[:, :width] + top[:, :width])

    def relax(y, s, y_prior):
        partial = r_v[OWN, y, s]
        if y_prior is not None:
            partial = partial - couple(y_prior, ny_v.at[OWN, y, s])
        left = split(partial)
        if s > 0:
            left = left + split(nz_v[OWN, y, s])
        both = lax.dot_general(
            jnp.concatenate(left, 0), jnp.concatenate(split(inv_v[OWN, y, s]), 0), (((1,), (1,)), ((), ())),
            preferred_element_type=F32,
        )
        return combine(both), combine(both[2 * vectors:]) if s > 0 else None

    def ends(tile):
        return [
            jnp.broadcast_to(tile[:, (d + 1) * seg_len - 1:(d + 1) * seg_len], (vectors, width))
            for d in range(comps)
        ]

    def climb(relaxed, prior):
        free, along = relaxed
        if prior is not None:
            free = free - add_up([e * along[d:d + 1, :] for d, e in enumerate(ends(prior))])
        return free

    def dense(tile):
        return jnp.concatenate(
            [
                jnp.concatenate(
                    [
                        jnp.where(diagonal, jnp.broadcast_to(part[d:d + 1], (seg_len, width)), 0.0).astype(BF16)
                        for d in range(comps)
                    ],
                    0,
                )
                for part in (p.astype(F32) for p in split(tile))
            ],
            1,
        )

    def product(h, y, s, with_y=True):
        high, low = split(inv_v[h, y, s])
        block = jnp.concatenate([jnp.concatenate([high, high], 1), jnp.concatenate([low, low], 1)], 0)
        head = jnp.concatenate(split(jnp.concatenate([r_v[h, y, s], nz_v[h, y, s]], 0)), 1)
        planes = [dense(nx_v[h, y, s])] + ([dense(ny_v[h, y, s])] if with_y else [])
        left = jnp.concatenate(planes + [head], 0)
        both = lax.dot_general(left, block, (((1,), (1,)), ((), ())), preferred_element_type=F32)
        total = both[:, :width] + both[:, width:]
        rows = len(planes) * width
        return total, total[0:rows], total[rows:rows + vectors], total[rows + vectors:]

    def keep(y, s, base, rows):
        high, low = split(rows)
        w_v[y, s, base:base + rows.shape[0], 0:width] = high
        w_v[y, s, base:base + rows.shape[0], width:2 * width] = low

    def fold(h, i, y, s, with_y=True):
        _, planes, k_v[i, y, s], g_v[i, y, s] = product(h, y, s, with_y)
        keep(y, s, i * 2 * width, planes)

    def fold_column(h, i):
        if h == OWN:
            arrive_blocks()

        def fold_chunk(p, carry):
            if h != OWN:
                arrive_chunk(p)
            for s in range(CHUNK):
                for y in range(yl):
                    fold(h, i, y, p * CHUNK + s)
            return carry

        lax.fori_loop(0, segs // CHUNK, fold_chunk, 0, unroll=CHUNK if h == OWN else 1)

    def fold_pair(y, s):
        lower_total, lower_planes, k_v[0, y, s], g_v[0, y, s] = product(0, y, s)
        keep(y, s, 0, lower_planes)
        _, upper_planes, upper_k, g_v[2, y, s] = product(OWN, y, s)
        keep(y, s, 4 * width, upper_planes[width:])
        high, low = split(upper_planes[:width])
        high_low = jnp.concatenate([high, low], 1)
        both = jnp.dot(
            jnp.concatenate(split(lower_total), 1), jnp.concatenate([high_low, high_low], 0),
            preferred_element_type=F32,
        )
        total = both[:, :width] + both[:, width:]
        keep(y, s, 2 * width, total[0:2 * width])
        k_v[1, y, s] = upper_k - total[2 * width:2 * width + vectors]
        g_v[1, y, s] = total[2 * width + vectors:]

    def along_z(parts, i, y, s):
        return add_up([p * g_v[i, y, s, d:d + 1, :] for d, p in enumerate(parts)])

    def stack(*tiles):
        parts = [split(t) for t in tiles]
        return jnp.concatenate(
            [jnp.concatenate([p[0] for p in parts], 1), jnp.concatenate([p[1] for p in parts], 1)], 0
        )

    def times(left, y, s, base, rows):
        return jnp.dot(left, w_v[y, s, base:base + rows, :], preferred_element_type=F32)

    def solve(cells, priors, sols, late=None):
        both = [
            times(stack(x), y, s, i * 2 * width, width) if y_prior is None
            else times(stack(x, y_prior), y, s, i * 2 * width, 2 * width)
            for (i, y, s), (x, y_prior) in zip(cells, priors)
        ]
        below = [ends(sols[i][y, s - 1]) if s > 0 else None for i, y, s in cells]
        if late is not None:
            late()
        values = []
        for (i, y, s), b, z in zip(cells, both, below):
            acc = k_v[i, y, s]
            if z is not None:
                acc = acc - along_z(z, i, y, s)
            values.append(acc - combine(b))
        return values

    def solve_pair(cells, priors, late, send_on):
        lefts = [(stack(x, y0), stack(y1)) for x, y0, y1 in priors]
        upper_both = [
            times(left, y, s, 2 * width, 2 * width) - times(left1, y, s, 4 * width, width)
            for (left, left1), (y, s) in zip(lefts, cells)
        ]
        lower_both = [times(left, y, s, 0, 2 * width) for (left, _), (y, s) in zip(lefts, cells)]
        below = [(ends(sol_v[y, s - 1]), ends(out[y, s - 1])) if s > 0 else None for y, s in cells]
        late()
        lower_accs = []
        for (y, s), upper_b, z in zip(cells, upper_both, below):
            lower_acc = k_v[0, y, s]
            upper_acc = k_v[1, y, s]
            if z is not None:
                lower_ends, upper_ends = z
                upper_acc = (upper_acc - along_z(upper_ends, 2, y, s)) + along_z(lower_ends, 1, y, s)
                lower_acc = lower_acc - along_z(lower_ends, 0, y, s)
            lower_accs.append(lower_acc)
            out[y, s] = upper_acc + combine(upper_b)
        send_on()
        for (y, s), lower_acc, lower_b in zip(cells, lower_accs, lower_both):
            sol_v[y, s] = lower_acc - combine(lower_b)

    def wave(t):
        return [(y, t - y) for y in range(yl) if 0 <= t - y < segs]

    def first_lower():
        start_loads()
        greet(OWN, 0)
        zpad[...] = jnp.zeros_like(zpad)
        arrive_small(OWN)
        prepare_r(OWN)
        arrive_blocks()
        relaxed = {(0, 0): relax(0, 0, None)}
        values = {}
        pl.semaphore_wait(barrier, 1)

        def pass_on(ready):
            for y, s in ready:
                values[y, s] = climb(relaxed[y, s], values.get((y, s - 1)))
                out[y, s] = values[y, s]
            for y, s in ready:
                send_x(y, s, OWN).start()

        pass_on([(0, 0)])
        prepare_z(OWN)
        prepare_y(OWN, True)
        for s in range(1, segs):
            relaxed[0, s] = relax(0, s, None)
        for t in range(1, segs + (yl - 1) * LAG):
            for y in range(1, yl):
                s = t - 1 - (y - 1) * LAG
                if 0 <= s < segs:
                    relaxed[y, s] = relax(y, s, values[y - 1, s])
            pass_on([(y, t - y * LAG) for y in range(yl) if 0 <= t - y * LAG < segs])
        if ny > 1:
            pl.semaphore_wait(ready_sem, 1)
            for dx in (OWN, 0):
                for s in range(segs):
                    send_y(out, 0, s, dx).start()
        drain(xin, send_sem.at[1])
        if ny > 1:
            drain(yin, send_sem.at[2])

    def first_upper():
        start_loads()
        greet(-OWN, 0)
        zpad[...] = jnp.zeros_like(zpad)
        arrive_small(OWN)
        prepare_r(OWN)
        for y in range(yl):
            for s, row in enumerate(relayout([cx_v[OWN, y, c] for c in range(comps)], seg_len)):
                nx_v[OWN, y, s] = row
        arrive_blocks()
        prepare_z(OWN)
        prepare_y(OWN)
        for s in range(segs):
            for y in range(yl):
                fold(OWN, 0, y, s, with_y=y > 0)
        pl.semaphore_wait(barrier, 1 + (groups > 1) + (groups == 2) + 2 * (ny > 1))
        if ny > 1:
            pl.semaphore_signal(ready_sem, inc=1, device_id=(gx - OWN, gy), device_id_type=MESH)
        def later(cells):
            if groups == 2:
                for y, s in cells:
                    send_x(y, s, OWN).start()
            for y, s in cells:
                if ny > 1 and y == yl - 1:
                    send_y(out, OWN, s, 0).start()

        for t in range(segs + yl - 1):
            cells = wave(t)
            take_x(cells)
            values = solve(
                [(0, y, s) for y, s in cells],
                [(xin[y, s], out[y - 1, s] if y > 0 else None) for y, s in cells],
                (out,), functools.partial(later, wave(t - 1)),
            )
            for (y, s), value in zip(cells, values):
                out[y, s] = value
            if groups > 1:
                for y, s in cells:
                    send_x(y, s, PAIR).start()
        later(wave(segs + yl - 2))
        if groups > 1:
            drain(xin, send_sem.at[0])
        if groups == 2:
            drain(xin, send_sem.at[1])
        if ny > 1:
            drain(yin.at[0], send_sem.at[2 + OWN])

    def clear():
        zpad[...] = jnp.zeros_like(zpad)

        @pl.when(group == 0)
        def _():
            xin[...] = jnp.zeros_like(xin)

        @pl.when(gy == 0)
        def _():
            yin[...] = jnp.zeros_like(yin)

    def wait_x(cells):
        if not cells:
            return

        @pl.when(group > 0)
        def _():
            take_x(cells)

    def wait_y(cells):
        if not cells:
            return

        @pl.when(gy > 0)
        def _():
            for h, s in cells:
                send_y(out, h, s, 0).wait_recv()

    def lower():
        start_loads()
        greet_if(jnp.logical_and(group > 0, jnp.logical_not(right)), -OWN, 0)
        greet_if(inner, OWN, 0)
        greet_if(gy > 0, OWN, -1)
        pl.semaphore_wait(barrier, 1)
        for k in range(count):
            push(k).start()
        for s in range(segs):
            push_block(s).start()
        clear()
        prepare(OWN)

        fold_column(OWN, 0)
        for t in range(segs + yl - 1):
            cells = wave(t)
            wait_x(cells)
            wait_y([(0, s) for y, s in cells if y == 0])
            values = solve(
                [(0, y, s) for y, s in cells],
                [(xin[y, s], yin[0, s] if y == 0 else out[y - 1, s]) for y, s in cells], (out,),
            )
            for (y, s), value in zip(cells, values):
                out[y, s] = value
        for k in range(count):
            push(k).wait_send()
        drain(inv_v.at[OWN], push_sem.at[count])

    def enter_upper():
        start_loads()
        greet(-OWN, 0)
        greet_if(group > 0, -PAIR, 0)
        greet_if(gy > 0, 0, -1)
        clear()

    def meet_upper():
        @pl.when(jnp.logical_or(right, above))
        def _():
            peers = jnp.where(right, 1, 0) + jnp.where(inner, 1, 0) + jnp.where(before_last, 1, 0)
            pl.semaphore_wait(barrier, peers + jnp.where(above, 2, 0))

    def send_down(cells):
        if cells:
            @pl.when(inner)
            def _():
                for y, s in cells:
                    hand_down(y, s).start()

    def send_right(done):
        if any(h == OWN for h, _, _ in done):
            @pl.when(right)
            def _():
                for h, y, s in done:
                    if h == OWN:
                        send_x(y, s, PAIR).start()

    def send_later(done):
        if any(y == yl - 1 for _, y, _ in done):
            @pl.when(above)
            def _():
                for h, y, s in done:
                    if y == yl - 1:
                        send_y(out if h == OWN else sol_v, h, s, 0).start()
                for h, y, s in done:
                    if y == yl - 1 and h != OWN:
                        send_y(sol_v, h, s, -OWN).start()

        if any(h == OWN for h, _, _ in done):
            @pl.when(before_last)
            def _():
                for h, y, s in done:
                    if h == OWN:
                        send_x(y, s, OWN).start()

    def leave_upper():
        for cond, kind in ((right, 0), (before_last, 1), (inner, 4)):
            pl.when(cond)(functools.partial(drain, xin, send_sem.at[kind]))

        @pl.when(above)
        def _():
            drain(yin, send_sem.at[2])
            drain(yin.at[0], send_sem.at[2 + OWN])

    def upper_plain():
        enter_upper()
        for h in reversed(range(PAIR)):
            prepare(h)
            fold_column(h, h)
        meet_upper()
        sols = (sol_v, out)

        def cells_at(t):
            return [(x, y, t - x - y) for x in reversed(range(PAIR)) for y in range(yl) if 0 <= t - x - y < segs]

        def late(t):
            send_down([(y, s) for x, y, s in cells_at(t) if x == 0])

        steps = segs + PAIR + yl - 2
        for t in range(steps):
            cells = cells_at(t)
            wait_x([(y, s) for x, y, s in cells if x == 0])
            wait_y([(x, s) for x, y, s in cells if y == 0])
            values = solve(
                cells,
                [
                    (xin[y, s] if x == 0 else sol_v[y, s], yin[x, s] if y == 0 else sols[x][y - 1, s])
                    for x, y, s in cells
                ],
                sols, functools.partial(late, t),
            )
            for (x, y, s), value in zip(cells, values):
                if x == OWN:
                    out[y, s] = value
            send_right(cells)
            for (x, y, s), value in zip(cells, values):
                if x != OWN:
                    sol_v[y, s] = value
            send_later(cells)
        leave_upper()

    def upper_folded():
        enter_upper()
        for h in reversed(range(PAIR)):
            prepare(h)

        arrive_blocks()

        def fold_all(p, carry):
            arrive_chunk(p)
            for s in range(CHUNK):
                for y in range(yl):
                    fold_pair(y, p * CHUNK + s)
            return carry

        lax.fori_loop(0, segs // CHUNK, fold_all, 0)
        meet_upper()

        def both_of(cells):
            return [(h, y, s) for y, s in cells for h in reversed(range(PAIR))]

        def late(t):
            send_down(wave(t))

        for t in range(segs + yl - 1):
            cells = wave(t)
            wait_x(cells)
            wait_y([(h, s) for y, s in cells if y == 0 for h in range(PAIR)])
            solve_pair(
                cells,
                [
                    (xin[y, s], yin[0, s] if y == 0 else sol_v[y - 1, s], yin[OWN, s] if y == 0 else out[y - 1, s])
                    for y, s in cells
                ],
                functools.partial(late, t), functools.partial(send_right, both_of(cells)),
            )
            send_later(both_of(cells))
        leave_upper()

    early = group < EARLY
    is_upper = jnp.logical_and(jnp.logical_not(origin), slot == OWN)
    pl.when(jnp.logical_and(origin, slot == 0))(first_lower)
    pl.when(jnp.logical_and(origin, slot == OWN))(first_upper)
    pl.when(jnp.logical_and(jnp.logical_not(origin), slot == 0))(lower)
    pl.when(jnp.logical_and(is_upper, early))(upper_plain)
    pl.when(jnp.logical_and(is_upper, jnp.logical_not(early)))(upper_folded)


def local(nx, ny, right_side, inverse_blocks, couple_x, couple_y, couple_z):
    _, yl, vectors, comps, cells = right_side.shape
    segs = inverse_blocks.shape[2]
    seg_len = cells // segs
    width = comps * seg_len
    lead = (PAIR, yl)
    rows = pltpu.VMEM(lead + (segs, comps, width), F32)
    vectors_v = pltpu.VMEM(lead + (segs, vectors, width), F32)
    vmem = pl.BlockSpec(memory_space=pltpu.VMEM)
    any_spec = pl.BlockSpec(memory_space=pl.ANY)
    solved = pl.pallas_call(
        functools.partial(kernel, nx, ny, (yl, vectors, comps, segs, seg_len)),
        out_shape=pltpu.VMEM((yl, segs, vectors, width), F32),
        in_specs=[any_spec] * 5,
        out_specs=vmem,
        scratch_shapes=[
            pltpu.VMEM(lead + right_side.shape[2:], F32),
            pltpu.VMEM(lead + inverse_blocks.shape[2:], F32),
            pltpu.VMEM(lead + couple_x.shape[2:], F32),
            pltpu.VMEM(lead + couple_y.shape[2:], F32),
            pltpu.VMEM(lead + couple_z.shape[2:], F32),
            pltpu.VMEM((yl, segs * seg_len, width), F32),
            pltpu.VMEM((yl, segs, 5 * width, 2 * width), BF16),
            vectors_v, rows, rows, rows, vectors_v,
            pltpu.VMEM((PAIR + 1, yl, segs, comps, width), F32),
            pltpu.VMEM((yl, segs, vectors, width), F32),
            pltpu.VMEM((PAIR, segs, vectors, width), F32),
            pltpu.VMEM((yl, segs, vectors, width), F32),
            pltpu.SemaphoreType.DMA((5,)),
            pltpu.SemaphoreType.DMA((5,)),
            pltpu.SemaphoreType.DMA((4 + segs // CHUNK,)),
            pltpu.SemaphoreType.DMA((segs + yl - 1,)),
            pltpu.SemaphoreType.DMA((PAIR, segs)),
            pltpu.SemaphoreType.DMA((5,)),
            pltpu.SemaphoreType.REGULAR,
        ],
        compiler_params=pltpu.CompilerParams(collective_id=0, has_side_effects=True),
        name="forward_solve",
    )(right_side, inverse_blocks, couple_x, couple_y, couple_z)
    return pl.pallas_call(
        functools.partial(finish, seg_len),
        out_shape=jax.ShapeDtypeStruct(right_side.shape, F32),
        in_specs=[vmem],
        out_specs=vmem,
        name="natural_layout",
    )(pltpu.with_memory_space_constraint(solved, pltpu.VMEM))


def solution(mesh):
    spec = P("gx", "gy", None, None, None)
    return jax.shard_map(
        functools.partial(local, mesh.shape["gx"], mesh.shape["gy"]),
        mesh=mesh, in_specs=(spec,) * 5, out_specs=spec, check_vma=False,
    )
```

```python
import functools
import jax
import jax.numpy as jnp
from jax import lax
from jax.experimental import pallas as pl
from jax.experimental.pallas import tpu as pltpu
from jax.sharding import PartitionSpec as P

MESH = pl.DeviceIdType.MESH
PAIR = 2
OWN = PAIR - 1
EARLY = 3
LAG = 3
CHUNK = 4
F32 = jnp.float32
BF16 = jnp.bfloat16


def roll(tile, shift):
    shift = shift % tile.shape[1]
    return tile if shift == 0 else pltpu.roll(tile, shift, 1)


def unskew(skewed, seg_len):
    count = len(skewed)
    group = lax.broadcasted_iota(jnp.int32, skewed[0].shape, 1) // seg_len
    rows = []
    for s in range(count):
        acc = skewed[0]
        for c in range(1, count):
            acc = jnp.where(group == (s + c) % count, skewed[c], acc)
        rows.append(roll(acc, -s * seg_len))
    return rows


def relayout(tiles, seg_len):
    return unskew([roll(t, c * seg_len) for c, t in enumerate(tiles)], seg_len)


def split(value):
    high = value.astype(BF16)
    return high, (value - high.astype(F32)).astype(BF16)


def add_up(terms):
    while len(terms) > 1:
        terms = [sum(terms[i:i + 2][1:], terms[i]) for i in range(0, len(terms), 2)]
    return terms[0]


def finish(seg_len, rows, out):
    for y in range(rows.shape[0]):
        tiles = relayout([rows[y, s] for s in range(rows.shape[1])], seg_len)
        for c, tile in enumerate(tiles):
            out[0, y, :, c, :] = tile


def kernel(
    nx, ny, dims,
    rhs, inv, cx, cy, cz, out,
    rhs_v, inv_v, cx_v, cy_v, cz_v, zpad, w_v, r_v, nx_v, ny_v, nz_v, k_v, g_v, xin, yin, sol_v,
    load_sem, push_sem, move_sem, x_sem, y_sem, send_sem, ready_sem,
):
    yl, vectors, comps, segs, seg_len = dims
    width = comps * seg_len
    gx = lax.axis_index("gx")
    gy = lax.axis_index("gy")
    group = gx // PAIR
    slot = gx % PAIR
    groups = nx // PAIR
    origin = jnp.logical_and(group == 0, gy == 0)
    right = group < groups - 1
    above = gy < ny - 1
    inner = jnp.logical_and(group > 0, right)
    before_last = group == groups - 2
    barrier = pltpu.get_barrier_semaphore()
    small = ((rhs, rhs_v), (cx, cx_v), (cy, cy_v), (cz, cz_v))
    count = len(small)

    def pieces(h):
        return [(a.at[0], b.at[h]) for a, b in small]

    def load(k):
        a, b = pieces(OWN)[k]
        return pltpu.make_async_copy(a, b, load_sem.at[k])

    def load_block(s):
        return pltpu.make_async_copy(inv.at[0, :, s], inv_v.at[OWN, :, s], load_sem.at[count])

    def push(k):
        a, b = pieces(0)[k]
        return pltpu.make_async_remote_copy(
            src_ref=a, dst_ref=b, send_sem=push_sem.at[k], recv_sem=move_sem.at[k],
            device_id=(gx + OWN, gy), device_id_type=MESH,
        )

    def push_block(s):
        return pltpu.make_async_remote_copy(
            src_ref=inv.at[0, :, s], dst_ref=inv_v.at[0, :, s], send_sem=push_sem.at[count],
            recv_sem=move_sem.at[count + s // CHUNK], device_id=(gx + OWN, gy), device_id_type=MESH,
        )

    def arrive(h, k):
        load(k).wait() if h == OWN else push(k).wait_recv()

    def drain(ref, sem):
        pltpu.make_async_copy(ref, ref, sem).wait()

    def arrive_blocks():
        drain(inv_v.at[OWN], load_sem.at[count])

    def arrive_chunk(p):
        drain(inv_v.at[0, :, 0:CHUNK], move_sem.at[count + p])

    def greet(dx, dy):
        pl.semaphore_signal(barrier, inc=1, device_id=(gx + dx, gy + dy), device_id_type=MESH)

    def greet_if(cond, dx, dy):
        pl.when(cond)(functools.partial(greet, dx, dy))

    def send(kind, src, dst, sem, dx, dy):
        return pltpu.make_async_remote_copy(
            src_ref=src, dst_ref=dst, send_sem=send_sem.at[kind], recv_sem=sem,
            device_id=(gx + dx, gy + dy), device_id_type=MESH,
        )

    def send_x(y, s, dx):
        return send(0 if dx == PAIR else 1, out.at[y, s], xin.at[y, s], x_sem.at[y + s], dx, 0)

    def send_y(src, h, s, dx):
        return send(2 + h, src.at[yl - 1, s], yin.at[h, s], y_sem.at[h, s], dx, 1)

    def hand_down(y, s):
        return send(4, xin.at[y, s], xin.at[y, s], x_sem.at[y + s], -OWN, 0)

    def take_x(cells):
        drain(xin.at[0, 0:len(cells)], x_sem.at[sum(cells[0])])

    def start_loads():
        for k in range(count):
            load(k).start()
        for s in range(segs):
            load_block(s).start()

    lane = lax.broadcasted_iota(jnp.int32, (comps, width), 1)
    diagonal = (
        lax.broadcasted_iota(jnp.int32, (seg_len, width), 0)
        == lax.broadcasted_iota(jnp.int32, (seg_len, width), 1) % seg_len
    )

    def arrive_small(h):
        for k in range(count):
            arrive(h, k)

    def prepare_r(h):
        for y in range(yl):
            for s, row in enumerate(relayout([rhs_v[h, y, :, c, :] for c in range(comps)], seg_len)):
                r_v[h, y, s] = row

    def prepare_y(h, turned=False):
        for y in range(yl):
            tiles = [pltpu.roll(cy_v[h, y, c], comps - c, 0) if turned and c else cy_v[h, y, c] for c in range(comps)]
            for s, row in enumerate(relayout(tiles, seg_len)):
                ny_v[h, y, s] = row

    def prepare_z(h):
        for y in range(yl):
            for s in range(segs):
                zpad[y, s * seg_len:s * seg_len + comps, 0:comps] = cz_v[h, y, s]
        flipped = [zpad[y].T[0:comps, :] for y in range(yl)]
        for y in range(yl):
            for s, row in enumerate(unskew([roll(flipped[y], c * (seg_len - 1)) for c in range(comps)], seg_len)):
                nz_v[h, y, s] = jnp.where(lane % seg_len == 0, row, 0.0)

    def prepare(h):
        arrive_small(h)
        prepare_z(h)
        prepare_r(h)
        for y in range(yl):
            for s, row in enumerate(relayout([cx_v[h, y, c] for c in range(comps)], seg_len)):
                nx_v[h, y, s] = row
        prepare_y(h)

    def couple(value, rows):
        return add_up([roll(value, -r * seg_len) * rows[r:r + 1, :] for r in range(comps)])

    def combine(both):
        top, bottom = both[0:vectors], both[vectors:2 * vectors]
        return (top[:, width:] + bottom[:, width:]) + (bottom[:, :width] + top[:, :width])

    def relax(y, s, y_prior):
        partial = r_v[OWN, y, s]
        if y_prior is not None:
            partial = partial - couple(y_prior, ny_v.at[OWN, y, s])
        left = split(partial)
        if s > 0:
            left = left + split(nz_v[OWN, y, s])
        both = lax.dot_general(
            jnp.concatenate(left, 0), jnp.concatenate(split(inv_v[OWN, y, s]), 0), (((1,), (1,)), ((), ())),
            preferred_element_type=F32,
        )
        return combine(both), combine(both[2 * vectors:]) if s > 0 else None

    def ends(tile):
        return [
            jnp.broadcast_to(tile[:, (d + 1) * seg_len - 1:(d + 1) * seg_len], (vectors, width))
            for d in range(comps)
        ]

    def climb(relaxed, prior):
        free, along = relaxed
        if prior is not None:
            free = free - add_up([e * along[d:d + 1, :] for d, e in enumerate(ends(prior))])
        return free

    def dense(tile):
        return jnp.concatenate(
            [
                jnp.concatenate(
                    [
                        jnp.where(diagonal, jnp.broadcast_to(part[d:d + 1], (seg_len, width)), 0.0).astype(BF16)
                        for d in range(comps)
                    ],
                    0,
                )
                for part in (p.astype(F32) for p in split(tile))
            ],
            1,
        )

    def product(h, y, s, with_y=True):
        high, low = split(inv_v[h, y, s])
        block = jnp.concatenate([jnp.concatenate([high, high], 1), jnp.concatenate([low, low], 1)], 0)
        head = jnp.concatenate(split(jnp.concatenate([r_v[h, y, s], nz_v[h, y, s]], 0)), 1)
        planes = [dense(nx_v[h, y, s])] + ([dense(ny_v[h, y, s])] if with_y else [])
        left = jnp.concatenate(planes + [head], 0)
        both = lax.dot_general(left, block, (((1,), (1,)), ((), ())), preferred_element_type=F32)
        total = both[:, :width] + both[:, width:]
        rows = len(planes) * width
        return total, total[0:rows], total[rows:rows + vectors], total[rows + vectors:]

    def keep(y, s, base, rows):
        high, low = split(rows)
        w_v[y, s, base:base + rows.shape[0], 0:width] = high
        w_v[y, s, base:base + rows.shape[0], width:2 * width] = low

    def fold(h, i, y, s, with_y=True):
        _, planes, k_v[i, y, s], g_v[i, y, s] = product(h, y, s, with_y)
        keep(y, s, i * 2 * width, planes)

    def fold_column(h, i):
        if h == OWN:
            arrive_blocks()

        def fold_chunk(p, carry):
            if h != OWN:
                arrive_chunk(p)
            for s in range(CHUNK):
                for y in range(yl):
                    fold(h, i, y, p * CHUNK + s)
            return carry

        lax.fori_loop(0, segs // CHUNK, fold_chunk, 0, unroll=1)

    def fold_pair(y, s):
        lower_total, lower_planes, k_v[0, y, s], g_v[0, y, s] = product(0, y, s)
        keep(y, s, 0, lower_planes)
        _, upper_planes, upper_k, g_v[2, y, s] = product(OWN, y, s)
        keep(y, s, 4 * width, upper_planes[width:])
        high, low = split(upper_planes[:width])
        high_low = jnp.concatenate([high, low], 1)
        both = jnp.dot(
            jnp.concatenate(split(lower_total), 1), jnp.concatenate([high_low, high_low], 0),
            preferred_element_type=F32,
        )
        total = both[:, :width] + both[:, width:]
        keep(y, s, 2 * width, total[0:2 * width])
        k_v[1, y, s] = upper_k - total[2 * width:2 * width + vectors]
        g_v[1, y, s] = total[2 * width + vectors:]

    def along_z(parts, i, y, s):
        return add_up([p * g_v[i, y, s, d:d + 1, :] for d, p in enumerate(parts)])

    def stack(*tiles):
        parts = [split(t) for t in tiles]
        return jnp.concatenate(
            [jnp.concatenate([p[0] for p in parts], 1), jnp.concatenate([p[1] for p in parts], 1)], 0
        )

    def times(left, y, s, base, rows):
        return jnp.dot(left, w_v[y, s, base:base + rows, :], preferred_element_type=F32)

    def solve(cells, priors, sols, late=None):
        both = [
            times(stack(x), y, s, i * 2 * width, width) if y_prior is None
            else times(stack(x, y_prior), y, s, i * 2 * width, 2 * width)
            for (i, y, s), (x, y_prior) in zip(cells, priors)
        ]
        below = [ends(sols[i][y, s - 1]) if s > 0 else None for i, y, s in cells]
        if late is not None:
            late()
        values = []
        for (i, y, s), b, z in zip(cells, both, below):
            acc = k_v[i, y, s]
            if z is not None:
                acc = acc - along_z(z, i, y, s)
            values.append(acc - combine(b))
        return values

    def solve_pair(cells, priors, late, send_on):
        lefts = [(stack(x, y0), stack(y1)) for x, y0, y1 in priors]
        upper_both = [
            times(left, y, s, 2 * width, 2 * width) - times(left1, y, s, 4 * width, width)
            for (left, left1), (y, s) in zip(lefts, cells)
        ]
        lower_both = [times(left, y, s, 0, 2 * width) for (left, _), (y, s) in zip(lefts, cells)]
        below = [(ends(sol_v[y, s - 1]), ends(out[y, s - 1])) if s > 0 else None for y, s in cells]
        late()
        lower_accs = []
        for (y, s), upper_b, z in zip(cells, upper_both, below):
            lower_acc = k_v[0, y, s]
            upper_acc = k_v[1, y, s]
            if z is not None:
                lower_ends, upper_ends = z
                upper_acc = (upper_acc - along_z(upper_ends, 2, y, s)) + along_z(lower_ends, 1, y, s)
                lower_acc = lower_acc - along_z(lower_ends, 0, y, s)
            lower_accs.append(lower_acc)
            out[y, s] = upper_acc + combine(upper_b)
        send_on()
        for (y, s), lower_acc, lower_b in zip(cells, lower_accs, lower_both):
            sol_v[y, s] = lower_acc - combine(lower_b)

    def wave(t):
        return [(y, t - y) for y in range(yl) if 0 <= t - y < segs]

    def first_lower():
        greet(OWN, 0)
        start_loads()
        zpad[...] = jnp.zeros_like(zpad)
        arrive_small(OWN)
        prepare_r(OWN)
        arrive_blocks()
        relaxed = {(0, 0): relax(0, 0, None)}
        values = {}
        pl.semaphore_wait(barrier, 1)

        def pass_on(ready):
            for y, s in ready:
                values[y, s] = climb(relaxed[y, s], values.get((y, s - 1)))
                out[y, s] = values[y, s]
            for y, s in ready:
                send_x(y, s, OWN).start()

        pass_on([(0, 0)])
        prepare_z(OWN)
        prepare_y(OWN, True)
        for s in range(1, segs):
            relaxed[0, s] = relax(0, s, None)
        for t in range(1, segs + (yl - 1) * LAG):
            for y in range(1, yl):
                s = t - 1 - (y - 1) * LAG
                if 0 <= s < segs:
                    relaxed[y, s] = relax(y, s, values[y - 1, s])
            pass_on([(y, t - y * LAG) for y in range(yl) if 0 <= t - y * LAG < segs])
        if ny > 1:
            pl.semaphore_wait(ready_sem, 1)
            for dx in (OWN, 0):
                for s in range(segs):
                    send_y(out, 0, s, dx).start()
        drain(xin, send_sem.at[1])
        if ny > 1:
            drain(yin, send_sem.at[2])

    def first_upper():
        greet(-OWN, 0)
        start_loads()
        zpad[...] = jnp.zeros_like(zpad)
        arrive_small(OWN)
        prepare_r(OWN)
        for y in range(yl):
            for s, row in enumerate(relayout([cx_v[OWN, y, c] for c in range(comps)], seg_len)):
                nx_v[OWN, y, s] = row
        arrive_blocks()
        prepare_z(OWN)
        prepare_y(OWN)
        for s in range(segs):
            for y in range(yl):
                fold(OWN, 0, y, s, with_y=y > 0)
        pl.semaphore_wait(barrier, 1 + (groups > 1) + (groups == 2) + 2 * (ny > 1))
        if ny > 1:
            pl.semaphore_signal(ready_sem, inc=1, device_id=(gx - OWN, gy), device_id_type=MESH)
        def later(cells):
            if groups == 2:
                for y, s in cells:
                    send_x(y, s, OWN).start()
            for y, s in cells:
                if ny > 1 and y == yl - 1:
                    send_y(out, OWN, s, 0).start()

        for t in range(segs + yl - 1):
            cells = wave(t)
            take_x(cells)
            values = solve(
                [(0, y, s) for y, s in cells],
                [(xin[y, s], out[y - 1, s] if y > 0 else None) for y, s in cells],
                (out,), functools.partial(later, wave(t - 1)),
            )
            for (y, s), value in zip(cells, values):
                out[y, s] = value
            if groups > 1:
                for y, s in cells:
                    send_x(y, s, PAIR).start()
        later(wave(segs + yl - 2))
        if groups > 1:
            drain(xin, send_sem.at[0])
        if groups == 2:
            drain(xin, send_sem.at[1])
        if ny > 1:
            drain(yin.at[0], send_sem.at[2 + OWN])

    def clear():
        zpad[...] = jnp.zeros_like(zpad)

        @pl.when(group == 0)
        def _():
            xin[...] = jnp.zeros_like(xin)

        @pl.when(gy == 0)
        def _():
            yin[...] = jnp.zeros_like(yin)

    def wait_x(cells):
        if not cells:
            return

        @pl.when(group > 0)
        def _():
            take_x(cells)

    def wait_y(cells):
        if not cells:
            return

        @pl.when(gy > 0)
        def _():
            for h, s in cells:
                send_y(out, h, s, 0).wait_recv()

    def lower():
        greet_if(jnp.logical_and(group > 0, jnp.logical_not(right)), -OWN, 0)
        greet_if(inner, OWN, 0)
        greet_if(gy > 0, OWN, -1)
        pl.semaphore_wait(barrier, 1)
        for k in range(count):
            push(k).start()
        for s in range(segs):
            push_block(s).start()
        start_loads()
        clear()
        prepare(OWN)

        fold_column(OWN, 0)
        for t in range(segs + yl - 1):
            cells = wave(t)
            wait_x(cells)
            wait_y([(0, s) for y, s in cells if y == 0])
            values = solve(
                [(0, y, s) for y, s in cells],
                [(xin[y, s], yin[0, s] if y == 0 else out[y - 1, s]) for y, s in cells], (out,),
            )
            for (y, s), value in zip(cells, values):
                out[y, s] = value
        for k in range(count):
            push(k).wait_send()
        drain(inv_v.at[OWN], push_sem.at[count])

    def enter_upper():
        greet(-OWN, 0)
        start_loads()
        greet_if(group > 0, -PAIR, 0)
        greet_if(gy > 0, 0, -1)
        clear()

    def meet_upper():
        @pl.when(jnp.logical_or(right, above))
        def _():
            peers = jnp.where(right, 1, 0) + jnp.where(inner, 1, 0) + jnp.where(before_last, 1, 0)
            pl.semaphore_wait(barrier, peers + jnp.where(above, 2, 0))

    def send_down(cells):
        if cells:
            @pl.when(inner)
            def _():
                for y, s in cells:
                    hand_down(y, s).start()

    def send_right(done):
        if any(h == OWN for h, _, _ in done):
            @pl.when(right)
            def _():
                for h, y, s in done:
                    if h == OWN:
                        send_x(y, s, PAIR).start()

    def send_later(done):
        if any(y == yl - 1 for _, y, _ in done):
            @pl.when(above)
            def _():
                for h, y, s in done:
                    if y == yl - 1:
                        send_y(out if h == OWN else sol_v, h, s, 0).start()
                for h, y, s in done:
                    if y == yl - 1 and h != OWN:
                        send_y(sol_v, h, s, -OWN).start()

        if any(h == OWN for h, _, _ in done):
            @pl.when(before_last)
            def _():
                for h, y, s in done:
                    if h == OWN:
                        send_x(y, s, OWN).start()

    def leave_upper():
        for cond, kind in ((right, 0), (before_last, 1), (inner, 4)):
            pl.when(cond)(functools.partial(drain, xin, send_sem.at[kind]))

        @pl.when(above)
        def _():
            drain(yin, send_sem.at[2])
            drain(yin.at[0], send_sem.at[2 + OWN])

    def upper_plain():
        enter_upper()
        for h in reversed(range(PAIR)):
            prepare(h)
            fold_column(h, h)
        meet_upper()
        sols = (sol_v, out)

        def cells_at(t):
            return [(x, y, t - x - y) for x in reversed(range(PAIR)) for y in range(yl) if 0 <= t - x - y < segs]

        def late(t):
            send_down([(y, s) for x, y, s in cells_at(t) if x == 0])

        steps = segs + PAIR + yl - 2
        for t in range(steps):
            cells = cells_at(t)
            wait_x([(y, s) for x, y, s in cells if x == 0])
            wait_y([(x, s) for x, y, s in cells if y == 0])
            values = solve(
                cells,
                [
                    (xin[y, s] if x == 0 else sol_v[y, s], yin[x, s] if y == 0 else sols[x][y - 1, s])
                    for x, y, s in cells
                ],
                sols, functools.partial(late, t),
            )
            for (x, y, s), value in zip(cells, values):
                if x == OWN:
                    out[y, s] = value
            send_right(cells)
            for (x, y, s), value in zip(cells, values):
                if x != OWN:
                    sol_v[y, s] = value
            send_later(cells)
        leave_upper()

    def upper_folded():
        enter_upper()
        for h in reversed(range(PAIR)):
            prepare(h)

        arrive_blocks()

        def fold_all(p, carry):
            for y in range(yl):
                fold_pair(y, p)
            return carry

        for p in range(segs // CHUNK):
            arrive_chunk(p)
            lax.fori_loop(p * CHUNK, (p + 1) * CHUNK, fold_all, 0, unroll=2)
        meet_upper()

        def both_of(cells):
            return [(h, y, s) for y, s in cells for h in reversed(range(PAIR))]

        def late(t):
            send_down(wave(t))

        for t in range(segs + yl - 1):
            cells = wave(t)
            wait_x(cells)
            wait_y([(h, s) for y, s in cells if y == 0 for h in range(PAIR)])
            solve_pair(
                cells,
                [
                    (xin[y, s], yin[0, s] if y == 0 else sol_v[y - 1, s], yin[OWN, s] if y == 0 else out[y - 1, s])
                    for y, s in cells
                ],
                functools.partial(late, t), functools.partial(send_right, both_of(cells)),
            )
            send_later(both_of(cells))
        leave_upper()

    early = group < EARLY
    is_upper = jnp.logical_and(jnp.logical_not(origin), slot == OWN)
    pl.when(jnp.logical_and(origin, slot == 0))(first_lower)
    pl.when(jnp.logical_and(origin, slot == OWN))(first_upper)
    pl.when(jnp.logical_and(jnp.logical_not(origin), slot == 0))(lower)
    pl.when(jnp.logical_and(is_upper, early))(upper_plain)
    pl.when(jnp.logical_and(is_upper, jnp.logical_not(early)))(upper_folded)


def local(nx, ny, right_side, inverse_blocks, couple_x, couple_y, couple_z):
    _, yl, vectors, comps, cells = right_side.shape
    segs = inverse_blocks.shape[2]
    seg_len = cells // segs
    width = comps * seg_len
    lead = (PAIR, yl)
    rows = pltpu.VMEM(lead + (segs, comps, width), F32)
    vectors_v = pltpu.VMEM(lead + (segs, vectors, width), F32)
    vmem = pl.BlockSpec(memory_space=pltpu.VMEM)
    any_spec = pl.BlockSpec(memory_space=pl.ANY)
    solved = pl.pallas_call(
        functools.partial(kernel, nx, ny, (yl, vectors, comps, segs, seg_len)),
        out_shape=pltpu.VMEM((yl, segs, vectors, width), F32),
        in_specs=[any_spec] * 5,
        out_specs=vmem,
        scratch_shapes=[
            pltpu.VMEM(lead + right_side.shape[2:], F32),
            pltpu.VMEM(lead + inverse_blocks.shape[2:], F32),
            pltpu.VMEM(lead + couple_x.shape[2:], F32),
            pltpu.VMEM(lead + couple_y.shape[2:], F32),
            pltpu.VMEM(lead + couple_z.shape[2:], F32),
            pltpu.VMEM((yl, segs * seg_len, width), F32),
            pltpu.VMEM((yl, segs, 5 * width, 2 * width), BF16),
            vectors_v, rows, rows, rows, vectors_v,
            pltpu.VMEM((PAIR + 1, yl, segs, comps, width), F32),
            pltpu.VMEM((yl, segs, vectors, width), F32),
            pltpu.VMEM((PAIR, segs, vectors, width), F32),
            pltpu.VMEM((yl, segs, vectors, width), F32),
            pltpu.SemaphoreType.DMA((5,)),
            pltpu.SemaphoreType.DMA((5,)),
            pltpu.SemaphoreType.DMA((4 + segs // CHUNK,)),
            pltpu.SemaphoreType.DMA((segs + yl - 1,)),
            pltpu.SemaphoreType.DMA((PAIR, segs)),
            pltpu.SemaphoreType.DMA((5,)),
            pltpu.SemaphoreType.REGULAR,
        ],
        compiler_params=pltpu.CompilerParams(collective_id=0, has_side_effects=True),
        name="forward_solve",
    )(right_side, inverse_blocks, couple_x, couple_y, couple_z)
    return pl.pallas_call(
        functools.partial(finish, seg_len),
        out_shape=jax.ShapeDtypeStruct(right_side.shape, F32),
        in_specs=[vmem],
        out_specs=vmem,
        name="natural_layout",
    )(pltpu.with_memory_space_constraint(solved, pltpu.VMEM))


def solution(mesh):
    spec = P("gx", "gy", None, None, None)
    return jax.shard_map(
        functools.partial(local, mesh.shape["gx"], mesh.shape["gy"]),
        mesh=mesh, in_specs=(spec,) * 5, out_specs=spec, check_vma=False,
    )
```
